256 devices in a mesh: grp: 32 (over y, z), row: 8 (over x, core).
Axes of the slice: x: 4, y: 4, z: 8, core: 2. Of those that a mesh axis runs over, the one named last changes fastest.
Arguments:
- block: bfloat16 [65536, 1024], P(('grp', 'row')), may hold values from -6 to 6
- degree: int32 [65536], P(('grp', 'row')), may hold values from 1 to 3
- tile_values: bfloat16 [16384, 128, 128], P(('grp', 'row')), may hold values from -0.1875 to 0.1875
- tile_rows: int32 [16384], P(('grp', 'row')), may hold values from 0 to 1
- tile_cols: int32 [16384], P(('grp', 'row')), may hold values from 0 to 47
- tile_count: int32 [256], P(('grp', 'row')), may hold values from 24 to 64, as said below
- send_tiles: int32 [256, 32], P(('grp', 'row')), may hold values from 0 to 1
Outputs:
- logs: bfloat16 [65536, 1024], P(('grp', 'row'))
- gram: float32 [32768, 1024], P(('grp', 'row'))
The draws below stay inside these ranges and needn't reach their ends.
Inputs may be any that keep to these rules, and one draw needn't show every extreme that they name: Slots of a device at positions tile_count or later are padding; some device has all 64 slots live.
All inputs are finite; a program needn't handle non-finite values.
Results may differ from the reference program's by a relative error of at most 0.014.
Values may be sent and summed in bfloat16 or wider, within the bound.
A program may use at most 128 MiB of HBM per device.

```python
import jax
import jax.numpy as jnp
from jax import lax

K = 1024
TILE = 128
ROWS_DEV = 256
SLOTS = 64
POWERS = 2
ROW_TILES = 2
NODES = 65536
SOURCES = 48
SLOTS_ALL = 16384
N_GRP = 32
N_ROW = 8


def draw_tile_count(key, part):
    first_key, second_key = jax.random.split(jax.random.fold_in(key, 7))
    devices = N_GRP * N_ROW
    drawn = jax.random.randint(first_key, (devices,), 0, SLOTS + 1)
    counts = jnp.minimum(SLOTS * 3 // 8 + drawn * drawn * 5 // (8 * SLOTS), SLOTS)
    chosen = jax.random.randint(second_key, (), 0, devices)
    counts = jnp.where(jnp.arange(devices) == chosen, SLOTS, counts)
    return counts.astype(jnp.int32)


def with_ends(values, stream_key, least, top_value):
    spot = [jax.random.randint(jax.random.fold_in(stream_key, axis), (), 0, length) for axis, length in enumerate(values.shape)]
    longest = values.shape.index(max(values.shape))
    beside = spot[:longest] + [(spot[longest] + 1) % values.shape[longest]] + spot[longest + 1:]
    return values.at[tuple(spot)].set(least).at[tuple(beside)].set(top_value)


def steps_of(key, extent, cuts, low, largest):
    gain, own = 1.0, jax.random.fold_in(key, 6)
    for axis_at, blocks in cuts:
        heights = jnp.exp(jax.random.uniform(jax.random.fold_in(own, axis_at), (blocks,), jnp.float32, low / len(cuts), largest / len(cuts)))
        gain = gain * jnp.repeat(heights, extent[axis_at] // blocks).reshape([-1 if axis == axis_at else 1 for axis in range(len(extent))])
    return gain


def centred(stream_key, extent, spread, reach, cuts=(), kind=jnp.bfloat16):
    gain = steps_of(stream_key, extent, cuts, -0.22, 0.18) if cuts else 1.0
    values = jax.random.normal(stream_key, extent, jnp.float32) * spread * gain
    return jnp.minimum(jnp.maximum(values, -reach), reach).astype(kind)


def setup_inputs(seed: int = 0) -> dict:
    key_of = jax.random.split(jax.random.key(seed), 8)
    return {
        "block": centred(key_of[0], (NODES, K), 1.0, 6.0, ((0, 256),)),
        "degree": with_ends(jax.random.randint(key_of[1], (NODES,), 1, 4), jax.random.fold_in(key_of[1], 1), 1, 3).astype(jnp.int32),
        "tile_values": centred(key_of[2], (SLOTS_ALL, TILE, TILE), (SLOTS * 16) ** -0.5, 0.1875, ((0, 256),)),
        "tile_rows": with_ends(jax.random.randint(key_of[3], (SLOTS_ALL,), 0, ROW_TILES), jax.random.fold_in(key_of[3], 1), 0, ROW_TILES - 1).astype(jnp.int32),
        "tile_cols": with_ends(jax.random.randint(key_of[4], (SLOTS_ALL,), 0, SOURCES), jax.random.fold_in(key_of[4], 1), 0, SOURCES - 1).astype(jnp.int32),
        "tile_count": draw_tile_count(jax.random.fold_in(key_of[7], 71), 0),
        "send_tiles": with_ends(jax.random.randint(key_of[6], (N_GRP * N_ROW, N_GRP), 0, ROW_TILES), jax.random.fold_in(key_of[6], 1), 0, ROW_TILES - 1).astype(jnp.int32),
    }


def column_tiles(tile_cols, send_tiles):
    row_tiles = ROWS_DEV // TILE
    slot_ids = jnp.arange(SLOTS * N_GRP * N_ROW, dtype=jnp.int32)
    device = slot_ids // SLOTS
    group = device // N_ROW
    member = device % N_ROW
    local_span = N_ROW * row_tiles
    source_group = jnp.maximum(tile_cols - local_span, 0)
    source_device = (source_group * N_ROW + member).astype(jnp.int32)
    remote = source_device * row_tiles + send_tiles[source_device, group]
    return jnp.where(tile_cols < local_span, group * local_span + tile_cols, remote).astype(jnp.int32)


def reference(block, degree, tile_values, tile_rows, tile_cols, tile_count, send_tiles):
    devices = N_GRP * N_ROW
    row_tiles = ROWS_DEV // TILE
    columns = column_tiles(tile_cols, send_tiles).reshape(devices, SLOTS)
    values = tile_values.reshape(devices, SLOTS, TILE, TILE)
    rows = tile_rows.reshape(devices, SLOTS)
    tile_ids = jnp.arange(row_tiles, dtype=jnp.int32)
    slot_pos = jnp.arange(SLOTS, dtype=jnp.int32)
    current = block
    power_sum = jnp.zeros(block.shape, jnp.float32)
    for power in range(POWERS):
        tiles_all = current.reshape(-1, TILE, K).astype(jnp.float32)

        def one_device(pieces):
            values_here, columns_here, rows_here, count_here = pieces
            picked = tiles_all[columns_here]
            products = jnp.einsum("sik,skf->sif", values_here.astype(jnp.float32), picked, precision=lax.Precision.HIGHEST)
            live_mask = slot_pos < count_here
            weights = ((rows_here[None, :] == tile_ids[:, None]) & live_mask[None, :]).astype(jnp.float32)
            return jnp.einsum("rs,sif->rif", weights, products, precision=lax.Precision.HIGHEST)

        summed = lax.map(one_device, (values, columns, rows, tile_count))
        current = (summed.reshape(-1, K) / degree[:, None].astype(jnp.float32)).astype(jnp.bfloat16)
        power_sum = power_sum + current.astype(jnp.float32)
    logs = jnp.log(jnp.maximum(3.0 * power_sum, 1.0)).astype(jnp.bfloat16)
    grouped = logs.reshape(N_GRP, N_ROW * ROWS_DEV, K)

    def group_gram(group_logs):
        return jnp.dot(group_logs.T, group_logs, preferred_element_type=jnp.float32)

    gram = lax.map(group_gram, grouped) / (N_ROW * ROWS_DEV)
    return logs, gram.reshape(N_GRP * K, K)
```

```python
import jax
import jax.numpy as jnp
from jax import lax
from jax.experimental import pallas as pl
from jax.experimental.pallas import tpu as pltpu
from jax.sharding import PartitionSpec as P

NX, NY, NZ = 4, 4, 8
TILE = 128
CHUNKS = 4
BACKLOG = 1.5
MESH = pl.DeviceIdType.MESH
SIGN = {"+": 1, "-": -1}


def build_kernel(rows_s, cols_s, count_s, send_s, degree_ref, values_hbm, row_ref, far_ref, bits_ref, div_ref, values, cells, sem):
    copy = pltpu.make_async_copy(values_hbm, values, sem)
    copy.start()
    codes = cells.shape[1]

    def clear(c, carry):
        for r in range(2):
            cells[r, c] = jnp.zeros((TILE, TILE), jnp.float32)
        return carry

    lax.fori_loop(0, codes, clear, 0)
    bits_ref[...] = jnp.zeros_like(bits_ref)
    for z in range(NZ):
        for y in range(NY):
            bit = send_s[0, y * NZ + z].astype(jnp.float32)
            bits_ref[z, pl.ds(y, 1), :] = jnp.full((1, TILE), bit, jnp.float32)
    for h in range(2):
        degrees = degree_ref[pl.ds(h, 1), :].astype(jnp.float32)
        div_ref[pl.ds(h * TILE, TILE), :] = jnp.broadcast_to(degrees, (TILE, TILE)).T
    copy.wait()

    def add(s, carry):
        r, c = rows_s[s], cols_s[s]
        cells[r, c] = cells[r, c] + values[s].astype(jnp.float32)
        return carry

    lax.fori_loop(0, count_s[0], add, 0)
    local = codes - NY * NZ
    for r in range(2):
        rows = pl.ds(r * TILE, TILE)
        for c in range(local):
            row_ref[rows, pl.ds(c * TILE, TILE)] = cells[r, c].astype(jnp.bfloat16)
        for y in range(NY):
            for z in range(NZ):
                far_ref[y, rows, pl.ds(z * TILE, TILE)] = cells[r, local + y * NZ + z].astype(jnp.bfloat16)


def build_dense(tile_rows, tile_cols, tile_count, send_tiles, degree, tile_values):
    slots = tile_values.shape[0]
    codes = 2 * 2 * NX + NY * NZ
    smem = pl.BlockSpec(memory_space=pltpu.SMEM)
    vmem = pl.BlockSpec(memory_space=pltpu.VMEM)
    return pl.pallas_call(
        build_kernel,
        out_shape=(
            jax.ShapeDtypeStruct((2 * TILE, 4 * NX * TILE), jnp.bfloat16),
            jax.ShapeDtypeStruct((NY, 2 * TILE, NZ * TILE), jnp.bfloat16),
            jax.ShapeDtypeStruct((NZ, 8, TILE), jnp.float32),
            jax.ShapeDtypeStruct((2 * TILE, TILE), jnp.float32),
        ),
        in_specs=[smem, smem, smem, smem, vmem, pl.BlockSpec(memory_space=pl.ANY)],
        out_specs=(vmem, vmem, vmem, vmem),
        scratch_shapes=[
            pltpu.VMEM((slots, TILE, TILE), jnp.bfloat16),
            pltpu.VMEM((2, codes, TILE, TILE), jnp.float32),
            pltpu.SemaphoreType.DMA,
        ],
        compiler_params=pltpu.CompilerParams(vmem_limit_bytes=24 * 1024 * 1024),
    )(tile_rows, tile_cols, tile_count, send_tiles, degree.reshape(2, TILE), tile_values)


def task_list(chunks, width):
    tasks = {}
    part = 1.0 / chunks

    def task(name, deps, link=None, units=0.0, cost=0.05, rank=0):
        tasks[name] = (deps, link, units, cost, rank)

    def got(name):
        return ("got", name)

    for k in range(1, NZ):
        task(("B", k), [], "z+", 0.01, 0.05, -20)
    for d in "+-":
        task(("W2a", d), [], "y" + d, 1, 0.05, -11)
        task(("W1", d), [], "y" + d, 2, 0.05, -10)
        task(("W2b", d), [got(("W2a", d))], "y" + d, 1, 0.05, -10)
    bits = [got(("B", k)) for k in range(1, NZ)]
    task(("E", "0"), bits, None, 0, 0.8, -5)
    task(("E", "+"), bits + [got(("W1", "-"))], None, 0, 0.8, -5)
    task(("E", "-"), bits + [got(("W1", "+"))], None, 0, 0.8, -5)
    task(("E", "2"), bits + [got(("W2b", "+")), got(("W2b", "-"))], None, 0, 0.8, -5)
    product = 2 * (2 * TILE) * (NZ * 2 * TILE) * width / 800e6
    gram_deps = []
    for p in range(3):
        for c in range(chunks):
            rank = p * chunks + c
            own = [("L", c)] if p == 0 else [("F", p - 1, c)]
            if p == 0:
                task(("L", c), [], None, 0, 0.05, rank)

            def ring(kind, axis, size):
                half = size // 2
                for d in "+-":
                    for s in range(1, half + 1):
                        deps = own if s == 1 else [got((kind, p, c, d, s - 1))]
                        task((kind, p, c, d, s), deps, axis + d, (2 if s < half else 1) * part, 0.05, rank)
                return [got((kind, p, c, d, s)) for d in "+-" for s in range(1, half + 1)]

            column = ring("Z", "z", NZ) + own if p < 2 else []
            row = ring("X", "x", NX) + own
            for q, deps, units in (
                ("0", own, 2),
                ("+", [got(("X", p, c, "+", 1))], 2),
                ("-", [got(("X", p, c, "-", 1))], 2),
                ("p", [got(("X", p, c, "+", 2))], 1),
                ("m", [got(("X", p, c, "-", 2))], 1),
            ):
                task(("D", p, c, q), deps, "d", units * part, 0.05, rank)
                row.append(got(("D", p, c, q)))
            if p == 2:
                gram_deps += row
                continue
            for j in "2+-0":
                task(("C", p, c, j), column + [("E", j)], None, 0, product, rank)
            task(("R", p, c), row + [("C", p, c, "0")], None, 0, product, rank)
            arrived = []
            for d in "+-":
                task(("Y1", p, c, d), [("C", p, c, "2")], "y" + d, part, 0.05, rank)
                task(("YB", p, c, d), [("C", p, c, d)], "y" + d, part, 0.05, rank)
                task(("A", p, c, d), [got(("Y1", p, c, d)), ("C", p, c, d)], None, 0, 0.3 * part * 2, rank)
                task(("YA", p, c, d), [("A", p, c, d)], "y" + d, part, 0.05, rank)
                arrived += [got(("YB", p, c, d)), got(("YA", p, c, d))]
            task(("F", p, c), arrived + [("R", p, c)] + own, None, 0, 1.6 * part, rank)
    task(("G",), gram_deps, None, 0, 2.0, 99)
    return tasks


def task_order(tasks, backlog):
    unit, latency = 5.62, {"d": 1.0}
    now, free, ended, landed, order = 3.0, {}, {}, {}, []
    left = dict(tasks)
    while left:
        best, best_key, soonest = None, None, 1e9
        for name, (deps, link, units, cost, rank) in left.items():
            ready = 0.0
            for dep in deps:
                at = landed.get(dep[1]) if dep[0] == "got" else ended.get(dep)
                if at is None:
                    ready = None
                    break
                ready = max(ready, at)
            if ready is None:
                continue
            if link is not None:
                ready = max(ready, free.get(link, 0.0) - backlog)
            if ready <= now + 1e-9:
                key = (link is None, rank, ready)
                if best is None or key < best_key:
                    best, best_key = name, key
            else:
                soonest = min(soonest, ready)
        if best is None:
            now = soonest
            continue
        deps, link, units, cost, rank = left.pop(best)
        now += cost
        ended[best] = now
        if link is not None:
            took = units * unit * (0.07 if link == "d" else 1.0)
            free[link] = max(now, free.get(link, 0.0)) + took
            landed[best] = free[link] + latency.get(link, 2.0)
        order.append(best)
    return order, now


def step_kernel(tasks, order, width, block_hbm, row_ref, far_ref, bits_ref, div_ref, logs_hbm, gram_ref,
                xz, xr, lg, wide, wr, stage, bits, p2, ps, pf, y1, yr, acc, flip, load_sem, out_sem, send_sem, recv_sem):
    chunks = xz.shape[1]
    g, r = lax.axis_index("grp"), lax.axis_index("row")
    me = (lax.div(g, NZ), lax.rem(g, NZ), lax.div(r, 2), lax.rem(r, 2))

    def moved(at, axis, by):
        y, z, x, k = at
        if axis == "y":
            return (lax.rem(y + by + NY, NY), z, x, k)
        if axis == "z":
            return (y, lax.rem(z + by + NZ, NZ), x, k)
        if axis == "x":
            return (y, z, lax.rem(x + by + NX, NX), k)
        return (y, z, x, 1 - k)

    def device(at):
        return (at[0] * NZ + at[1], at[2] * 2 + at[3])

    def rows(first, size):
        return pl.ds(pl.multiple_of(first, TILE), size)

    number = {}
    for name in tasks:
        if tasks[name][1] is not None:
            number[name] = len(number)

    def target(name, at):
        kind = name[0]
        if kind == "B":
            return moved(at, "z", name[1])
        if kind == "D":
            return moved(at, "k", 1)
        axis = {"Z": "z", "X": "x"}.get(kind, "y")
        return moved(at, axis, SIGN[name[1] if kind[0] == "W" else name[3]])

    def source(name, at):
        kind = name[0]
        if kind == "B":
            return moved(at, "z", -name[1])
        if kind == "D":
            return moved(at, "k", 1)
        axis = {"Z": "z", "X": "x"}.get(kind, "y")
        return moved(at, axis, -SIGN[name[1] if kind[0] == "W" else name[3]])

    def span(first, half):
        if half is None:
            return rows(first, 2 * TILE)
        return rows(first + half * TILE, TILE)

    def ends(name, at):
        kind = name[0]
        if kind == "B":
            return bits_ref.at[moved(at, "z", name[1])[1]], bits.at[at[1]]
        if kind == "W1":
            d = name[1]
            return far_ref.at[moved(at, "y", SIGN[d])[0]], wr.at[0 if d == "-" else 1]
        if kind == "W2a":
            h = 0 if name[1] == "+" else 1
            return far_ref.at[moved(at, "y", 2)[0], pl.ds(h * TILE, TILE)], stage.at[h]
        if kind == "W2b":
            h = 0 if name[1] == "+" else 1
            return stage.at[h], wr.at[2, pl.ds(h * TILE, TILE)]
        p, c, d = name[1:4]
        if kind == "Z":
            s = name[4]
            first = moved(at, "z", -SIGN[d] * (s - 1))[1] * (2 * TILE)
            half = None if s < NZ // 2 else (0 if d == "+" else 1)
            ref = xz.at[p, c, span(first, half)]
            return ref, ref
        if kind in "XD":
            whole = xr.at[p] if p < 2 else lg
            if kind == "X":
                s = name[4]
                from_x = moved(at, "x", -SIGN[d] * (s - 1))[2]
                half = None if s < NX // 2 else (0 if d == "+" else 1)
            else:
                by, half = {"0": (0, None), "+": (-1, None), "-": (1, None), "p": (-2, 0), "m": (2, 1)}[d]
                from_x = moved(at, "x", by)[2]
            ref = whole.at[c, span((from_x * 2 + at[3]) * (2 * TILE), half)]
            return ref, ref
        i = 0 if d == "+" else 1
        top, low = pl.ds(i * TILE, TILE), pl.ds((1 - i) * TILE, TILE)
        if kind == "Y1":
            return p2.at[p, c, top], y1.at[p, c, i]
        if kind == "YA":
            return ps.at[p, c, i, top], yr.at[p, c, i, top]
        return ps.at[p, c, i, low], yr.at[p, c, i, low]

    def descriptor(name, at, to):
        src, dst = ends(name, at)
        i = number[name]
        return pltpu.make_async_remote_copy(
            src_ref=src, dst_ref=dst, send_sem=send_sem.at[i], recv_sem=recv_sem.at[i],
            device_id=device(to), device_id_type=MESH)

    def arrival(name):
        origin = source(name, me)
        dst = ends(name, origin)[1]
        i = number[name]
        return pltpu.make_async_remote_copy(
            src_ref=dst, dst_ref=dst, send_sem=send_sem.at[i], recv_sem=recv_sem.at[i],
            device_id=device(origin), device_id_type=MESH)

    own_z = rows(me[1] * (2 * TILE), 2 * TILE)
    own_r = rows(r * (2 * TILE), 2 * TILE)

    def loads(c):
        piece = block_hbm.at[:, pl.ds(c * width, width)]
        return (pltpu.make_async_copy(piece, xz.at[0, c, own_z], load_sem.at[c, 0]),
                pltpu.make_async_copy(piece, xr.at[0, c, own_r], load_sem.at[c, 1]))

    def store(c):
        return pltpu.make_async_copy(lg.at[c, own_r], logs_hbm.at[:, pl.ds(c * width, width)], out_sem.at[c])

    for c in range(chunks):
        for copy in loads(c):
            copy.start()
    bits[me[1]] = bits_ref[me[1]]
    peers = [moved(me, "z", k) for k in range(1, NZ)]
    peers += [moved(me, "y", 1), moved(me, "y", -1), moved(me, "x", 1), moved(me, "x", -1), moved(me, "k", 1)]
    barrier = pltpu.get_barrier_semaphore()
    for peer in peers:
        pl.semaphore_signal(barrier, inc=1, device_id=device(peer), device_id_type=MESH)
    pl.semaphore_wait(barrier, len(peers))

    def dot(a, b):
        return jnp.dot(a, b, preferred_element_type=jnp.float32)

    def widen(j):
        slot = "0+-2".index(j)
        y = moved(me, "y", {"0": 0, "+": 1, "-": -1, "2": 2}[j])[0]
        for z in range(NZ):
            bit = bits[z, pl.ds(y, 1), :]
            if j == "0":
                piece = far_ref[me[0], :, pl.ds(z * TILE, TILE)]
            else:
                piece = wr[slot - 1, :, pl.ds(z * TILE, TILE)]
            piece = piece.astype(jnp.float32)
            wide[slot, :, pl.ds(z * 2 * TILE, TILE)] = (piece * (1.0 - bit)).astype(jnp.bfloat16)
            wide[slot, :, pl.ds(z * 2 * TILE + TILE, TILE)] = (piece * bit).astype(jnp.bfloat16)

    def run(name):
        kind = name[0]
        if kind == "L":
            for copy in loads(name[1]):
                copy.wait()
        elif kind == "E":
            widen(name[1])
        elif kind == "C":
            p, c, j = name[1:]
            made = dot(wide["0+-2".index(j)], xz[p, c])
            if j == "0":
                acc[p, c] = made
            elif j == "2":
                p2[p, c] = made.astype(jnp.bfloat16)
            else:
                i = 0 if j == "+" else 1
                pf[p, c, i] = made[i * TILE:(i + 1) * TILE]
                ps[p, c, i, pl.ds((1 - i) * TILE, TILE)] = made[(1 - i) * TILE:(2 - i) * TILE].astype(jnp.bfloat16)
        elif kind == "R":
            p, c = name[1:]
            acc[p, c] += dot(row_ref[...], xr[p, c])
        elif kind == "A":
            p, c, d = name[1:]
            i = 0 if d == "+" else 1
            ps[p, c, i, pl.ds(i * TILE, TILE)] = (pf[p, c, i] + y1[p, c, i].astype(jnp.float32)).astype(jnp.bfloat16)
        elif kind == "F":
            p, c = name[1:]
            summed = acc[p, c] + yr[p, c, 0].astype(jnp.float32) + yr[p, c, 1].astype(jnp.float32)
            divisor = jnp.concatenate([div_ref[...]] * (width // TILE), axis=1)
            power = (summed / divisor).astype(jnp.bfloat16)
            if p == 0:
                xz[1, c, own_z] = power
                xr[1, c, own_r] = power
            else:
                total = xr[1, c, own_r].astype(jnp.float32) + power.astype(jnp.float32)
                lg[c, own_r] = jnp.log(jnp.maximum(3.0 * total, 1.0)).astype(jnp.bfloat16)
                store(c).start()
        else:
            per = width // TILE
            mine = pl.ds(pl.multiple_of(lax.rem(r, per) * TILE, TILE), TILE)
            flip[...] = lg[lax.div(r, per), :, mine].T
            for c in range(chunks):
                gram_ref[:, pl.ds(c * width, width)] = dot(flip[...], lg[c]) * (1.0 / (lg.shape[1]))

    waited = set()
    for name in order:
        for dep in tasks[name][0]:
            if dep[0] == "got" and dep[1] not in waited:
                waited.add(dep[1])
                arrival(dep[1]).wait_recv()
        if name in number:
            descriptor(name, me, target(name, me)).start()
        else:
            run(name)
    for c in range(chunks):
        store(c).wait()
    for name in number:
        descriptor(name, me, target(name, me)).wait_send()


def body(block, degree, tile_values, tile_rows, tile_cols, tile_count, send_tiles):
    near, far, bits, divisor = build_dense(tile_rows, tile_cols, tile_count, send_tiles, degree, tile_values)
    rows_here, features = block.shape
    chunks = CHUNKS
    width = features // chunks
    tasks = task_list(chunks, width)
    order, _ = task_order(tasks, BACKLOG)
    sends = sum(1 for t in tasks.values() if t[1] is not None)
    vmem = pl.BlockSpec(memory_space=pltpu.VMEM)
    hbm = pl.BlockSpec(memory_space=pl.ANY)
    column = NZ * 2 * TILE
    bf16, f32 = jnp.bfloat16, jnp.float32
    ranks = 2 * NX

    def kernel(*refs):
        step_kernel(tasks, order, width, *refs)

    return pl.pallas_call(
        kernel,
        out_shape=(
            jax.ShapeDtypeStruct((rows_here, features), bf16),
            jax.ShapeDtypeStruct((features // ranks, features), f32),
        ),
        in_specs=[hbm, vmem, vmem, vmem, vmem],
        out_specs=(hbm, vmem),
        scratch_shapes=[
            pltpu.VMEM((2, chunks, column, width), bf16),
            pltpu.VMEM((2, chunks, ranks * 2 * TILE, width), bf16),
            pltpu.VMEM((chunks, ranks * 2 * TILE, width), bf16),
            pltpu.VMEM((4, 2 * TILE, column), bf16),
            pltpu.VMEM((3, 2 * TILE, NZ * TILE), bf16),
            pltpu.VMEM((2, TILE, NZ * TILE), bf16),
            pltpu.VMEM((NZ, 8, TILE), f32),
            pltpu.VMEM((2, chunks, 2 * TILE, width), bf16),
            pltpu.VMEM((2, chunks, 2, 2 * TILE, width), bf16),
            pltpu.VMEM((2, chunks, 2, TILE, width), f32),
            pltpu.VMEM((2, chunks, 2, TILE, width), bf16),
            pltpu.VMEM((2, chunks, 2, 2 * TILE, width), bf16),
            pltpu.VMEM((2, chunks, 2 * TILE, width), f32),
            pltpu.VMEM((TILE, ranks * 2 * TILE), bf16),
            pltpu.SemaphoreType.DMA((chunks, 2)),
            pltpu.SemaphoreType.DMA((chunks,)),
            pltpu.SemaphoreType.DMA((sends,)),
            pltpu.SemaphoreType.DMA((sends,)),
        ],
        compiler_params=pltpu.CompilerParams(
            collective_id=0, has_side_effects=True, vmem_limit_bytes=52 * 1024 * 1024),
    )(block, near, far, bits, divisor)


def solution(mesh):
    placed = (
        P(("grp", "row"), None),
        P(("grp", "row")),
        P(("grp", "row"), None, None),
        P(("grp", "row")),
        P(("grp", "row")),
        P(("grp", "row")),
        P(("grp", "row"), None),
    )
    return jax.shard_map(
        body,
        mesh=mesh,
        in_specs=placed,
        out_specs=(P(("grp", "row"), None), P(("grp", "row"), None)),
        check_vma=False,
    )
```

```python
import jax
import jax.numpy as jnp
from jax import lax
from jax.experimental import pallas as pl
from jax.experimental.pallas import tpu as pltpu
from jax.sharding import PartitionSpec as P

NX, NY, NZ = 4, 4, 8
TILE = 128
WIDTHS = (256, 256, 256, 128, 128)
BACKLOG = 0.5
RATE = 460e6
LIMIT = 46 * 1024 * 1024
BUILD_LIMIT = 20 * 1024 * 1024
BITS_LATE = 4.0
LATE = {"z": 2.3, "y": 2.8, "x": 5.0, "d": 4.0, "X": 2.5, "D": 1.5}
MESH = pl.DeviceIdType.MESH
ORDER = (
    48, 53, 49, 8, 18, 19, 23, 78, 0, 108, 11, 4, 83, 50, 59, 121, 9, 27, 12, 1, 5, 24, 20, 113, 7, 61, 54, 13,
    138, 87, 57, 139, 89, 2, 10, 79, 21, 25, 119, 29, 3, 143, 6, 93, 63, 55, 51, 120, 22, 26, 80, 149, 15, 91, 28, 84,
    117, 31, 32, 90, 140, 30, 56, 144, 52, 16, 58, 17, 35, 62, 43, 147, 39, 109, 14, 36, 85, 81, 141, 44, 150, 40, 65, 73,
    69, 88, 60, 41, 45, 122, 42, 114, 46, 110, 34, 66, 74, 153, 33, 70, 145, 37, 86, 71, 64, 82, 38, 75, 72, 76, 115, 142,
    47, 111, 172, 92, 67, 146, 168, 176, 68, 118, 77, 205, 201, 152, 197, 148, 94, 95, 116, 96, 103, 104, 112, 124, 151, 99, 173, 207,
    155, 100, 157, 169, 156, 163, 202, 177, 160, 198, 127, 105, 125, 106, 101, 129, 102, 126, 159, 174, 133, 170, 97, 98, 165, 203, 166, 199,
    178, 180, 107, 164, 135, 130, 208, 206, 161, 131, 154, 226, 230, 234, 236, 162, 211, 171, 136, 132, 210, 158, 175, 167, 284, 288, 123, 134,
    200, 292, 128, 204, 137, 231, 227, 184, 188, 240, 294, 192, 185, 259, 255, 293, 237, 179, 193, 189, 285, 213, 221, 181, 217, 289, 214, 232,
    222, 228, 235, 194, 182, 265, 260, 190, 191, 298, 256, 212, 195, 183, 215, 219, 218, 223, 290, 238, 263, 295, 286, 224, 209, 220, 269, 186,
    233, 229, 187, 196, 241, 261, 257, 216, 313, 266, 225, 291, 287, 315, 242, 250, 246, 243, 323, 258, 247, 262, 251, 321, 244, 239, 300, 308,
    304, 301, 248, 249, 252, 253, 264, 271, 279, 316, 314, 275, 305, 325, 319, 299, 272, 310, 309, 267, 297, 324, 296, 322, 311, 306, 307, 276,
    280, 268, 245, 254, 331, 329, 281, 282, 277, 278, 270, 326, 302, 273, 327, 303, 312, 320, 347, 345, 274, 333, 283, 339, 337, 330, 317, 318,
    332, 348, 346, 340, 338, 334, 342, 341, 350, 336, 349, 351, 335, 343, 328, 352, 344, 353,
)
SIGN = {"+": 1, "-": -1}


def build_kernel(cell_s, count_s, values, row_ref, far_ref, cells):
    codes = cells.shape[0] // 2

    def clear(c, carry):
        for r in range(2):
            cells[r * codes + c] = jnp.zeros((TILE, TILE), jnp.float32)
        return carry

    lax.fori_loop(0, codes, clear, 0)

    def add(s, carry):
        cell = cell_s[s]
        cells[cell] = cells[cell] + values[s].astype(jnp.float32)
        return carry

    lax.fori_loop(0, count_s[0], add, 0)
    local = codes - NY * NZ
    for r in range(2):
        rows = pl.ds(r * TILE, TILE)
        for c in range(local):
            row_ref[rows, pl.ds(c * TILE, TILE)] = cells[r * codes + c].astype(jnp.bfloat16)
        for y in range(NY):
            for z in range(NZ):
                far_ref[y, rows, pl.ds(z * TILE, TILE)] = cells[r * codes + local + y * NZ + z].astype(jnp.bfloat16)


def build_dense(tile_rows, tile_cols, tile_count, tile_values):
    codes = 2 * 2 * NX + NY * NZ
    smem = pl.BlockSpec(memory_space=pltpu.SMEM)
    vmem = pl.BlockSpec(memory_space=pltpu.VMEM)
    return pl.pallas_call(
        build_kernel,
        out_shape=(
            jax.ShapeDtypeStruct((2 * TILE, 4 * NX * TILE), jnp.bfloat16),
            jax.ShapeDtypeStruct((NY, 2 * TILE, NZ * TILE), jnp.bfloat16),
        ),
        in_specs=[smem, smem, vmem],
        out_specs=(vmem, vmem),
        scratch_shapes=[pltpu.VMEM((2 * codes, TILE, TILE), jnp.float32)],
        compiler_params=pltpu.CompilerParams(vmem_limit_bytes=BUILD_LIMIT),
    )(tile_rows * codes + tile_cols, tile_count, tile_values)


def task_list(widths):
    tasks = {}
    chunks = len(widths)

    def task(name, deps, link=None, units=0.0, cost=0.05, rank=0):
        late = LATE.get("X" if name[0] == "X" and name[1] == 2 else "D" if name[0] == "D" and name[1] == 2 else (link or "z")[0])
        late = BITS_LATE if name[0] == "B" else late
        tasks[name] = (deps, link, units, cost, rank, late)

    def got(name):
        return ("got", name)

    hops = [("B", d, s) for d in "+-" for s in range(1, NZ // 2 + (d == "+"))]
    for _, d, s in hops:
        task(("B", d, s), [] if s == 1 else [got(("B", d, s - 1))], "z" + d, 0.01, 0.05, -20)
    task(("H",), [], None, 0, 0.3, 50)
    for d in "+-":
        task(("W2a", d), [], "y" + d, 1, 0.05, -11)
        task(("W1", d), [], "y" + d, 2, 0.05, -10)
        task(("W2b", d), [got(("W2a", d))], "y" + d, 1, 0.05, -10)
    bits = [got(hop) for hop in hops] + [("H",)]
    task(("E", "0"), bits, None, 0, 0.4, -5)
    task(("E", "+"), bits + [got(("W1", "-"))], None, 0, 0.4, -5)
    task(("E", "-"), bits + [got(("W1", "+"))], None, 0, 0.4, -5)
    task(("E", "2"), bits + [got(("W2b", "+")), got(("W2b", "-"))], None, 0, 0.4, -5)
    gram_deps = []
    for p in range(3):
        for c in range(chunks):
            rank = p * chunks + c
            part = widths[c] / sum(widths)
            product = 2 * (2 * TILE) * (NZ * 2 * TILE) * max(widths[c], 192) / RATE
            own = [("L", c)] if p == 0 else [("F", p - 1, c)]
            if p == 0:
                task(("L", c), [], None, 0, 0.05, rank)

            def ring(kind, axis, size):
                half = size // 2
                for d in "+-":
                    for s in range(1, half + 1):
                        deps = own if s == 1 else [got((kind, p, c, d, s - 1))]
                        task((kind, p, c, d, s), deps, axis + d, (2 if s < half else 1) * part, 0.05, rank)
                return [got((kind, p, c, d, s)) for d in "+-" for s in range(1, half + 1)]

            column = ring("Z", "z", NZ) + own if p < 2 else []
            row = ring("X", "x", NX) + own
            for q, deps, units in (
                ("0", own, 2),
                ("+", [got(("X", p, c, "+", 1))], 2),
                ("-", [got(("X", p, c, "-", 1))], 2),
                ("f", [got(("X", p, c, "+", 2)), got(("X", p, c, "-", 2))], 2),
            ):
                task(("D", p, c, q), deps, "d", units * part, 0.05, rank)
                row.append(got(("D", p, c, q)))
            if p == 2:
                gram_deps += row
                continue
            task(("C", p, c, "2"), column + [("E", "2")], None, 0, product, rank)
            task(("C", p, c, "s"), column + [("E", j) for j in "+-"], None, 0, 2.1 * product, rank)
            task(("C", p, c, "0"), column + [("E", "0")], None, 0, product * 0.95, rank)
            task(("R", p, c), row + [("C", p, c, "0"), ("H",)], None, 0, product * 1.2, rank)
            arrived = []
            for d in "+-":
                task(("Y1", p, c, d), [("C", p, c, "2")], "y" + d, part, 0.05, rank)
                task(("YB", p, c, d), [("C", p, c, "s")], "y" + d, part, 0.05, rank)
                task(("A", p, c, d), [got(("Y1", p, c, d)), ("C", p, c, "s")], None, 0, 0.05, rank)
                task(("YA", p, c, d), [("A", p, c, d)], "y" + d, part, 0.05, rank)
                arrived += [got(("YB", p, c, d)), got(("YA", p, c, d))]
            task(("F", p, c), arrived + [("R", p, c), ("H",)] + own, None, 0, 0.15, rank)
    task(("G",), gram_deps, None, 0, 0.95, 99)
    return tasks


def task_order(tasks, backlog):
    unit = 5.62
    now, free, ended, landed, order = 3.0, {}, {}, {}, []
    left = dict(tasks)
    while left:
        best, best_key, soonest = None, None, 1e9
        for name, (deps, link, units, cost, rank, late) in left.items():
            ready = 0.0
            for dep in deps:
                at = landed.get(dep[1]) if dep[0] == "got" else ended.get(dep)
                if at is None:
                    ready = None
                    break
                ready = max(ready, at)
            if ready is None:
                continue
            if link is not None:
                ready = max(ready, free.get(link, 0.0) - backlog)
            if ready <= now + 1e-9:
                key = (link is None, rank, ready)
                if best is None or key < best_key:
                    best, best_key = name, key
            else:
                soonest = min(soonest, ready)
        if best is None:
            now = soonest
            continue
        deps, link, units, cost, rank, late = left.pop(best)
        now += cost
        ended[best] = now
        if link is not None:
            took = units * unit * (0.07 if link == "d" else 1.0)
            free[link] = max(now, free.get(link, 0.0)) + took
            landed[best] = free[link] + late
        order.append(best)
    return order, now


def step_kernel(tasks, order, widths, block_hbm, row_ref, far_ref, send_hbm, degree_hbm, logs_hbm, gram_hbm,
                per_chunk, wide, wr, stage, bits, flip, send_ref, degree_ref, div_ref, gram_ref,
                load_sem, misc_sem, out_sem, send_sem, recv_sem):
    chunks = len(widths)
    offsets = [sum(widths[:c]) for c in range(chunks)]
    xz, xr, p2, ps, pf, y1, yr, acc, lg = per_chunk
    g, r = lax.axis_index("grp"), lax.axis_index("row")
    me = (lax.div(g, NZ), lax.rem(g, NZ), lax.div(r, 2), lax.rem(r, 2))

    def moved(at, axis, by):
        y, z, x, k = at
        if axis == "y":
            return (lax.rem(y + by + NY, NY), z, x, k)
        if axis == "z":
            return (y, lax.rem(z + by + NZ, NZ), x, k)
        if axis == "x":
            return (y, z, lax.rem(x + by + NX, NX), k)
        return (y, z, x, 1 - k)

    def device(at):
        return (at[0] * NZ + at[1], at[2] * 2 + at[3])

    def rows(first, size):
        return pl.ds(pl.multiple_of(first, TILE), size)

    number = {}
    for name in tasks:
        if tasks[name][1] is not None:
            number[name] = len(number)

    def arrives_with(name):
        if name[0] == "D":
            return ("D", name[1], name[2])
        if name[0] in ("YA", "YB"):
            return ("Y", name[1], name[2])
        if (name[0], name[-1]) in (("Z", NZ // 2), ("X", NX // 2)):
            return (name[0], name[1], name[2])
        return name

    together = {}
    for name in number:
        together.setdefault(arrives_with(name), []).append(name)
    slot = {key: i for i, key in enumerate(together)}
    groups = {}
    for name in number:
        key = (name[0][0],) if name[0][0] in "WB" else ({"Z": "Z", "X": "X", "D": "X"}.get(name[0], "Y"), name[1], name[2])
        groups.setdefault(key, len(groups))

    def group_of(name):
        key = (name[0][0],) if name[0][0] in "WB" else ({"Z": "Z", "X": "X", "D": "X"}.get(name[0], "Y"), name[1], name[2])
        return groups[key]

    def target(name, at):
        kind = name[0]
        if kind == "D":
            return moved(at, "k", 1)
        axis = {"Z": "z", "X": "x", "B": "z"}.get(kind, "y")
        return moved(at, axis, SIGN[name[1] if kind[0] in "WB" else name[3]])

    def source(name, at):
        kind = name[0]
        if kind == "D":
            return moved(at, "k", 1)
        axis = {"Z": "z", "X": "x", "B": "z"}.get(kind, "y")
        return moved(at, axis, -SIGN[name[1] if kind[0] in "WB" else name[3]])

    def span(first, half):
        if half is None:
            return rows(first, 2 * TILE)
        return rows(first + half * TILE, TILE)

    def ends(name, at):
        kind = name[0]
        if kind == "B":
            ref = bits.at[moved(at, "z", -SIGN[name[1]] * (name[2] - 1))[1]]
            return ref, ref
        if kind == "W1":
            d = name[1]
            return far_ref.at[moved(at, "y", SIGN[d])[0]], wr.at[0 if d == "-" else 1]
        if kind == "W2a":
            h = 0 if name[1] == "+" else 1
            return far_ref.at[moved(at, "y", 2)[0], pl.ds(h * TILE, TILE)], stage.at[h]
        if kind == "W2b":
            h = 0 if name[1] == "+" else 1
            return stage.at[h], wr.at[2, pl.ds(h * TILE, TILE)]
        p, c, d = name[1:4]
        if kind == "Z":
            s = name[4]
            first = moved(at, "z", -SIGN[d] * (s - 1))[1] * (2 * TILE)
            half = None if s < NZ // 2 else (0 if d == "+" else 1)
            ref = xz[p][c].at[span(first, half)]
            return ref, ref
        if kind in "XD":
            whole = xr[p][c] if p < 2 else lg[0][c]
            if kind == "X":
                s = name[4]
                from_x = moved(at, "x", -SIGN[d] * (s - 1))[2]
                half = None if s < NX // 2 else (0 if d == "+" else 1)
            else:
                by, half = {"0": 0, "+": -1, "-": 1, "f": 2}[d], None
                from_x = moved(at, "x", by)[2]
            ref = whole.at[span((from_x * 2 + at[3]) * (2 * TILE), half)]
            return ref, ref
        i = 0 if d == "+" else 1
        top, low = pl.ds(i * TILE, TILE), pl.ds((1 - i) * TILE, TILE)
        if kind == "Y1":
            return p2[p][c].at[top], y1[p][c].at[i]
        if kind == "YA":
            return ps[p][c].at[i, top], yr[p][c].at[i, top]
        return ps[p][c].at[i, low], yr[p][c].at[i, low]

    def descriptor(name, at, to):
        src, dst = ends(name, at)
        return pltpu.make_async_remote_copy(
            src_ref=src, dst_ref=dst, send_sem=send_sem.at[group_of(name)], recv_sem=recv_sem.at[slot[arrives_with(name)]],
            device_id=device(to), device_id_type=MESH)

    def arrival(name):
        key = arrives_with(name)
        if len(together[key]) == 1:
            dst = ends(name, source(name, me))[1]
        else:
            kind, p, c = key
            dst = xr[0][c].at[pl.ds(0, {"D": 8, "Y": 4, "Z": 2, "X": 2}[kind] * TILE)]
        return pltpu.make_async_remote_copy(
            src_ref=dst, dst_ref=dst, send_sem=send_sem.at[0], recv_sem=recv_sem.at[slot[key]],
            device_id=device(source(name, me)), device_id_type=MESH)

    own_z = rows(me[1] * (2 * TILE), 2 * TILE)
    own_r = rows(r * (2 * TILE), 2 * TILE)

    def loads(c):
        piece = block_hbm.at[:, pl.ds(offsets[c], widths[c])]
        return (pltpu.make_async_copy(piece, xz[0][c].at[own_z], load_sem.at[c, 0]),
                pltpu.make_async_copy(piece, xr[0][c].at[own_r], load_sem.at[c, 1]))

    def emit(c):
        cols = pl.ds(offsets[c], widths[c])
        return pltpu.make_async_copy(gram_ref.at[:, cols], gram_hbm.at[:, cols], out_sem.at[c, 1])

    def store(c):
        return pltpu.make_async_copy(lg[0][c].at[own_r], logs_hbm.at[:, pl.ds(offsets[c], widths[c])], out_sem.at[c, 0])

    for c in range(chunks):
        for copy in loads(c):
            copy.start()
    send_copy = pltpu.make_async_copy(send_hbm, send_ref, misc_sem.at[0])
    degree_copy = pltpu.make_async_copy(degree_hbm, degree_ref, misc_sem.at[1])
    for copy in (send_copy, degree_copy):
        copy.start()
    peers = [moved(me, axis, by) for axis in "zyx" for by in (1, -1)] + [moved(me, "k", 1)]
    barrier = pltpu.get_barrier_semaphore()
    for peer in peers:
        pl.semaphore_signal(barrier, inc=1, device_id=device(peer), device_id_type=MESH)
    send_copy.wait()
    bits[me[1]] = jnp.zeros(bits.shape[1:], bits.dtype)
    bits[me[1], pl.ds(0, 1), pl.ds(0, NY * NZ)] = send_ref[...]
    pl.semaphore_wait(barrier, len(peers))

    def dot(a, b):
        return jnp.dot(a, b, preferred_element_type=jnp.float32)

    def widen(j):
        slot = "0+-2".index(j)
        out = pl.ds("2+-0".index(j) * 2 * TILE, 2 * TILE)
        y = moved(me, "y", {"0": 0, "+": 1, "-": -1, "2": 2}[j])[0]
        for z in range(NZ):
            told = bits[z, pl.ds(0, 1), :].astype(jnp.float32)
            lane = lax.broadcasted_iota(jnp.int32, told.shape, 1)
            bit = jnp.sum(jnp.where(lane == y * NZ + me[1], told, 0.0), axis=1, keepdims=True)
            if j == "0":
                piece = far_ref[me[0], :, pl.ds(z * TILE, TILE)]
            else:
                piece = wr[slot - 1, :, pl.ds(z * TILE, TILE)]
            piece = piece.astype(jnp.float32)
            wide[out, pl.ds(z * 2 * TILE, TILE)] = (piece * (1.0 - bit)).astype(jnp.bfloat16)
            wide[out, pl.ds(z * 2 * TILE + TILE, TILE)] = (piece * bit).astype(jnp.bfloat16)

    def run(name):
        kind = name[0]
        if kind == "L":
            for copy in loads(name[1]):
                copy.wait()
        elif kind == "E":
            widen(name[1])
        elif kind == "H":
            degree_copy.wait()
            for h in range(2):
                degrees = degree_ref[pl.ds(h, 1), :].astype(jnp.float32)
                div_ref[pl.ds(h * TILE, TILE), :] = jnp.broadcast_to(degrees, (TILE, TILE)).T
        elif kind == "C":
            p, c, j = name[1:]
            if j == "0":
                acc[p][c][...] = dot(wide[pl.ds(6 * TILE, 2 * TILE), :], xz[p][c][...])
            elif j == "2":
                p2[p][c][...] = dot(wide[pl.ds(0, 2 * TILE), :], xz[p][c][...]).astype(jnp.bfloat16)
            else:
                made = dot(wide[pl.ds(2 * TILE, 4 * TILE), :], xz[p][c][...])
                for i in range(2):
                    part = made[2 * i * TILE:(2 + 2 * i) * TILE]
                    pf[p][c][i] = part[i * TILE:(i + 1) * TILE]
                    ps[p][c][i, pl.ds((1 - i) * TILE, TILE)] = part[(1 - i) * TILE:(2 - i) * TILE].astype(jnp.bfloat16)
        elif kind == "R":
            p, c = name[1:]
            acc[p][c][...] += dot(row_ref[...], xr[p][c][...])
        elif kind == "A":
            p, c, d = name[1:]
            i = 0 if d == "+" else 1
            ps[p][c][i, pl.ds(i * TILE, TILE)] = (pf[p][c][i] + y1[p][c][i].astype(jnp.float32)).astype(jnp.bfloat16)
        elif kind == "F":
            p, c = name[1:]
            summed = acc[p][c][...] + yr[p][c][0].astype(jnp.float32) + yr[p][c][1].astype(jnp.float32)
            divisor = jnp.concatenate([div_ref[...]] * (widths[c] // TILE), axis=1)
            power = (summed / divisor).astype(jnp.bfloat16)
            if p == 0:
                xz[1][c][own_z] = power
                xr[1][c][own_r] = power
            else:
                total = xr[1][c][own_r].astype(jnp.float32) + power.astype(jnp.float32)
                lg[0][c][own_r] = jnp.log(jnp.maximum(3.0 * total, 1.0)).astype(jnp.bfloat16)
                store(c).start()
        else:
            for c in range(chunks):
                first, count = offsets[c] // TILE, widths[c] // TILE

                @pl.when((r >= first) & (r < first + count))
                def _():
                    mine = pl.ds(pl.multiple_of((r - first) * TILE, TILE), TILE)
                    flip[...] = lg[0][c][:, mine].T

            for c in range(chunks):
                made = dot(flip[...], lg[0][c][...])
                gram_ref[:, pl.ds(offsets[c], widths[c])] = made * (1.0 / flip.shape[1])
                emit(c).start()

    waited = set()
    for name in order:
        for dep in tasks[name][0]:
            if dep[0] == "got" and dep[1] not in waited:
                waited.update(together[arrives_with(dep[1])])
                arrival(dep[1]).wait_recv()
        if name in number:
            descriptor(name, me, target(name, me)).start()
        else:
            run(name)
    for c in range(chunks):
        store(c).wait()
        emit(c).wait()
    for key, i in groups.items():
        if key[0] == "W":
            sent = far_ref
        elif key[0] == "B":
            sent = bits.at[pl.ds(0, NZ - 1)]
        else:
            kind, p, c = key
            sent = xz[0][c].at[pl.ds(0, (6 if kind == "Y" else 14) * TILE)]
        pltpu.make_async_remote_copy(
            src_ref=sent, dst_ref=sent, send_sem=send_sem.at[i], recv_sem=recv_sem.at[0],
            device_id=device(moved(me, "k", 1)), device_id_type=MESH).wait_send()


def body(block, degree, tile_values, tile_rows, tile_cols, tile_count, send_tiles):
    near, far = build_dense(tile_rows, tile_cols, tile_count, tile_values)
    rows_here, features = block.shape
    widths = WIDTHS
    tasks = task_list(widths)
    names = list(tasks)
    order = [names[i] for i in ORDER]
    hbm = pl.BlockSpec(memory_space=pl.ANY)
    vmem = pl.BlockSpec(memory_space=pltpu.VMEM)
    column, ranks = NZ * 2 * TILE, 2 * NX
    bf16, f32 = jnp.bfloat16, jnp.float32

    def kernel(*refs):
        step_kernel(tasks, order, widths, *refs)

    def each(lead, dtype):
        return [pltpu.VMEM((*lead, w), dtype) for w in widths]

    both = [
        each((column,), bf16), each((ranks * 2 * TILE,), bf16), each((2 * TILE,), bf16), each((2, 2 * TILE), bf16),
        each((2, TILE), f32), each((2, TILE), bf16), each((2, 2 * TILE), bf16), each((2 * TILE,), f32),
    ]
    return pl.pallas_call(
        kernel,
        out_shape=(
            jax.ShapeDtypeStruct((rows_here, features), bf16),
            jax.ShapeDtypeStruct((features // ranks, features), f32),
        ),
        in_specs=[hbm, vmem, vmem, hbm, hbm],
        out_specs=(hbm, hbm),
        scratch_shapes=[
            [[b, b] for b in both] + [[each((ranks * 2 * TILE,), bf16)]],
            pltpu.VMEM((4 * 2 * TILE, column), bf16),
            pltpu.VMEM((3, 2 * TILE, NZ * TILE), bf16),
            pltpu.VMEM((2, TILE, NZ * TILE), bf16),
            pltpu.VMEM((NZ, 8, TILE), jnp.int32),
            pltpu.VMEM((TILE, ranks * 2 * TILE), bf16),
            pltpu.VMEM((1, NY * NZ), jnp.int32),
            pltpu.VMEM((2, TILE), jnp.int32),
            pltpu.VMEM((2 * TILE, TILE), f32),
            pltpu.VMEM((features // ranks, features), f32),
            pltpu.SemaphoreType.DMA((len(widths), 2)),
            pltpu.SemaphoreType.DMA((2,)),
            pltpu.SemaphoreType.DMA((len(widths), 2)),
            pltpu.SemaphoreType.DMA((8 * len(widths) + 2,)),
            pltpu.SemaphoreType.DMA((14 * 2 * len(widths) + 4 * len(widths) + 13,)),
        ],
        compiler_params=pltpu.CompilerParams(
            collective_id=0, has_side_effects=True, vmem_limit_bytes=LIMIT),
    )(block, near, far, send_tiles, degree.reshape(2, TILE))


def solution(mesh):
    placed = (
        P(("grp", "row"), None),
        P(("grp", "row")),
        P(("grp", "row"), None, None),
        P(("grp", "row")),
        P(("grp", "row")),
        P(("grp", "row")),
        P(("grp", "row"), None),
    )
    return jax.shard_map(
        body,
        mesh=mesh,
        in_specs=placed,
        out_specs=(P(("grp", "row"), None), P(("grp", "row"), None)),
        check_vma=False,
    )
```

```python
import jax
import jax.numpy as jnp
from jax import lax
from jax.experimental import pallas as pl
from jax.experimental.pallas import tpu as pltpu
from jax.sharding import PartitionSpec as P

NX, NY, NZ = 4, 4, 8
TILE = 128
WIDTHS = (256, 256, 256, 128, 128)
BACKLOG = 0.5
RATE = 460e6
LIMIT = 46 * 1024 * 1024
BUILD_LIMIT = 20 * 1024 * 1024
BITS_LATE = 4.0
LATE = {"z": 2.3, "y": 2.8, "x": 5.0, "d": 4.0, "X": 2.5, "D": 1.5}
MESH = pl.DeviceIdType.MESH
ORDER = (
    47, 52, 18, 19, 8, 23, 105, 27, 134, 31, 11, 76, 48, 12, 29, 4, 58, 56, 0, 77, 7, 53, 20, 9, 24, 57, 30, 1,
    143, 28, 49, 145, 5, 135, 60, 54, 110, 59, 32, 6, 10, 25, 81, 114, 21, 85, 2, 87, 13, 50, 139, 34, 119, 3, 22, 26,
    106, 33, 62, 63, 55, 146, 78, 111, 140, 51, 82, 15, 17, 35, 40, 43, 116, 90, 107, 16, 36, 144, 136, 41, 61, 14, 44, 112,
    79, 141, 39, 42, 150, 45, 86, 64, 37, 88, 108, 72, 83, 137, 69, 38, 46, 167, 163, 66, 65, 80, 70, 73, 148, 115, 142, 84,
    149, 117, 68, 74, 138, 109, 91, 113, 175, 71, 67, 171, 92, 164, 168, 93, 89, 101, 75, 195, 173, 191, 98, 151, 122, 118, 94, 99,
    127, 130, 124, 165, 169, 159, 172, 176, 203, 120, 121, 147, 102, 156, 95, 97, 100, 123, 103, 196, 201, 192, 152, 131, 96, 199, 128, 126,
    153, 170, 129, 166, 174, 177, 132, 155, 104, 223, 158, 219, 161, 197, 125, 193, 160, 227, 229, 133, 179, 247, 257, 205, 184, 157, 181, 154,
    187, 251, 220, 178, 224, 255, 200, 180, 162, 202, 188, 198, 194, 287, 279, 275, 183, 233, 185, 189, 285, 248, 186, 252, 221, 225, 230, 207,
    204, 212, 215, 260, 276, 228, 182, 190, 283, 305, 280, 258, 253, 286, 303, 209, 289, 249, 208, 211, 222, 234, 226, 214, 217, 256, 206, 216,
    213, 232, 277, 259, 281, 210, 250, 254, 306, 288, 284, 235, 240, 243, 236, 218, 311, 278, 313, 244, 282, 241, 263, 271, 304, 268, 231, 264,
    261, 239, 245, 242, 237, 291, 296, 269, 299, 292, 315, 290, 272, 267, 312, 273, 314, 270, 297, 262, 300, 238, 246, 319, 321, 295, 298, 301,
    265, 309, 266, 274, 329, 327, 316, 293, 294, 302, 337, 335, 320, 323, 307, 322, 330, 328, 336, 338, 333, 325, 332, 310, 341, 340, 324, 317,
    318, 339, 326, 308, 331, 334, 342, 343,
)
SIGN = {"+": 1, "-": -1}


def build_kernel(cell_s, count_s, values, row_ref, far_ref, cells):
    codes = cells.shape[0] // 2

    def clear(c, carry):
        for r in range(2):
            cells[r * codes + c] = jnp.zeros((TILE, TILE), jnp.float32)
        return carry

    lax.fori_loop(0, codes, clear, 0)

    def add(s, carry):
        cell = cell_s[s]
        cells[cell] = cells[cell] + values[s].astype(jnp.float32)
        return carry

    lax.fori_loop(0, count_s[0], add, 0)
    local = codes - NY * NZ
    for r in range(2):
        rows = pl.ds(r * TILE, TILE)
        for c in range(local):
            row_ref[rows, pl.ds(c * TILE, TILE)] = cells[r * codes + c].astype(jnp.bfloat16)
        for y in range(NY):
            for z in range(NZ):
                far_ref[y, rows, pl.ds(z * TILE, TILE)] = cells[r * codes + local + y * NZ + z].astype(jnp.bfloat16)


def build_dense(tile_rows, tile_cols, tile_count, tile_values):
    codes = 2 * 2 * NX + NY * NZ
    smem = pl.BlockSpec(memory_space=pltpu.SMEM)
    vmem = pl.BlockSpec(memory_space=pltpu.VMEM)
    return pl.pallas_call(
        build_kernel,
        out_shape=(
            jax.ShapeDtypeStruct((2 * TILE, 4 * NX * TILE), jnp.bfloat16),
            jax.ShapeDtypeStruct((NY, 2 * TILE, NZ * TILE), jnp.bfloat16),
        ),
        in_specs=[smem, smem, vmem],
        out_specs=(vmem, vmem),
        scratch_shapes=[pltpu.VMEM((2 * codes, TILE, TILE), jnp.float32)],
        compiler_params=pltpu.CompilerParams(vmem_limit_bytes=BUILD_LIMIT),
    )(tile_rows * codes + tile_cols, tile_count, tile_values)


def task_list(widths):
    tasks = {}
    chunks = len(widths)

    def task(name, deps, link=None, units=0.0, cost=0.05, rank=0):
        late = LATE.get("X" if name[0] == "X" and name[1] == 2 else "D" if name[0] == "D" and name[1] == 2 else (link or "z")[0])
        late = BITS_LATE if name[0] == "B" else late
        tasks[name] = (deps, link, units, cost, rank, late)

    def got(name):
        return ("got", name)

    hops = [("B", d, s) for d in "+-" for s in range(1, NZ // 2 + (d == "+"))]
    for _, d, s in hops:
        task(("B", d, s), [] if s == 1 else [got(("B", d, s - 1))], "z" + d, 0.01, 0.05, -20)
    task(("H",), [], None, 0, 0.3, 50)
    for d in "+-":
        task(("W2a", d), [], "y" + d, 1, 0.05, -11)
        task(("W1", d), [], "y" + d, 2, 0.05, -10)
        task(("W2b", d), [got(("W2a", d))], "y" + d, 1, 0.05, -10)
    bits = [got(hop) for hop in hops] + [("H",)]
    task(("E", "0"), bits, None, 0, 0.4, -5)
    task(("E", "+"), bits + [got(("W1", "-"))], None, 0, 0.4, -5)
    task(("E", "-"), bits + [got(("W1", "+"))], None, 0, 0.4, -5)
    task(("E", "2"), bits + [got(("W2b", "+")), got(("W2b", "-"))], None, 0, 0.4, -5)
    gram_deps = []
    for p in range(3):
        for c in range(chunks):
            rank = p * chunks + c
            part = widths[c] / sum(widths)
            product = 2 * (2 * TILE) * (NZ * 2 * TILE) * max(widths[c], 190) / RATE
            own = [("L", c)] if p == 0 else [("F", p - 1, c)]
            if p == 0:
                task(("L", c), [], None, 0, 0.05, rank)

            def ring(kind, axis, size):
                half = size // 2
                for d in "+-":
                    for s in range(1, half + 1):
                        deps = own if s == 1 else [got((kind, p, c, d, s - 1))]
                        task((kind, p, c, d, s), deps, axis + d, (2 if s < half else 1) * part, 0.05, rank)
                return [got((kind, p, c, d, s)) for d in "+-" for s in range(1, half + 1)]

            column = ring("Z", "z", NZ) + own if p < 2 else []
            row = ring("X", "x", NX) + own
            for q, deps, units in (
                ("0", own, 2),
                ("+", [got(("X", p, c, "+", 1))], 2),
                ("-", [got(("X", p, c, "-", 1))], 2),
                ("f", [got(("X", p, c, "+", 2)), got(("X", p, c, "-", 2))], 2),
            ):
                task(("D", p, c, q), deps, "d", units * part, 0.05, rank)
                row.append(got(("D", p, c, q)))
            if p == 2:
                gram_deps += row
                continue
            task(("C", p, c, "2"), column + [("E", "2")], None, 0, product, rank)
            task(("C", p, c, "s"), column + [("E", j) for j in "+-"], None, 0, 2.1 * product, rank)
            task(("C", p, c, "0"), column + [("E", "0")], None, 0, product * 0.95, rank)
            task(("R", p, c), row + [("C", p, c, "0"), ("H",)], None, 0, product * 1.2, rank)
            arrived = []
            crossed = [got(("Y1", p, c, d)) for d in "+-"]
            task(("A", p, c), crossed + [("C", p, c, "s")], None, 0, 0.1, rank)
            for d in "+-":
                task(("Y1", p, c, d), [("C", p, c, "2")], "y" + d, part, 0.05, rank)
                task(("YB", p, c, d), [("C", p, c, "s")], "y" + d, part, 0.05, rank)
                task(("YA", p, c, d), [("A", p, c)], "y" + d, part, 0.05, rank)
                arrived += [got(("YB", p, c, d)), got(("YA", p, c, d))]
            task(("F", p, c), arrived + [("R", p, c), ("H",)] + own, None, 0, 0.15, rank)
    task(("G",), gram_deps, None, 0, 0.95, 99)
    return tasks


def task_order(tasks, backlog):
    unit = 5.62
    now, free, ended, landed, order = 3.0, {}, {}, {}, []
    left = dict(tasks)
    while left:
        best, best_key, soonest = None, None, 1e9
        for name, (deps, link, units, cost, rank, late) in left.items():
            ready = 0.0
            for dep in deps:
                at = landed.get(dep[1]) if dep[0] == "got" else ended.get(dep)
                if at is None:
                    ready = None
                    break
                ready = max(ready, at)
            if ready is None:
                continue
            if link is not None:
                ready = max(ready, free.get(link, 0.0) - backlog)
            if ready <= now + 1e-9:
                key = (link is None, rank, ready)
                if best is None or key < best_key:
                    best, best_key = name, key
            else:
                soonest = min(soonest, ready)
        if best is None:
            now = soonest
            continue
        deps, link, units, cost, rank, late = left.pop(best)
        now += cost
        ended[best] = now
        if link is not None:
            took = units * unit * (0.07 if link == "d" else 1.0)
            free[link] = max(now, free.get(link, 0.0)) + took
            landed[best] = free[link] + late
        order.append(best)
    return order, now


def step_kernel(tasks, order, widths, block_hbm, row_ref, far_ref, send_hbm, degree_hbm, logs_ref, gram_ref,
                per_chunk, wide, wr, stage, bits, flip, send_ref, degree_ref, div_ref,
                load_sem, misc_sem, send_sem, recv_sem):
    chunks = len(widths)
    offsets = [sum(widths[:c]) for c in range(chunks)]
    xz, xr, p2, ps, pf, y1, yr, acc, lg = per_chunk
    g, r = lax.axis_index("grp"), lax.axis_index("row")
    me = (lax.div(g, NZ), lax.rem(g, NZ), lax.div(r, 2), lax.rem(r, 2))

    def moved(at, axis, by):
        y, z, x, k = at
        if axis == "y":
            return (lax.rem(y + by + NY, NY), z, x, k)
        if axis == "z":
            return (y, lax.rem(z + by + NZ, NZ), x, k)
        if axis == "x":
            return (y, z, lax.rem(x + by + NX, NX), k)
        return (y, z, x, 1 - k)

    def device(at):
        return (at[0] * NZ + at[1], at[2] * 2 + at[3])

    def rows(first, size):
        return pl.ds(pl.multiple_of(first, TILE), size)

    number = {}
    for name in tasks:
        if tasks[name][1] is not None:
            number[name] = len(number)

    def arrives_with(name):
        if name[0] == "D":
            return ("D", name[1], name[2])
        if name[0] == "Y1":
            return ("Y1", name[1], name[2])
        if name[0] in ("YA", "YB"):
            return ("Y", name[1], name[2])
        if (name[0], name[-1]) in (("Z", NZ // 2), ("X", NX // 2)):
            return (name[0], name[1], name[2])
        return name

    together = {}
    for name in number:
        together.setdefault(arrives_with(name), []).append(name)
    slot = {key: i for i, key in enumerate(together)}
    groups = {}
    for name in number:
        key = (name[0][0],) if name[0][0] in "WB" else ({"Z": "Z", "X": "X", "D": "X"}.get(name[0], "Y"), name[1])
        groups.setdefault(key, len(groups))

    def group_of(name):
        key = (name[0][0],) if name[0][0] in "WB" else ({"Z": "Z", "X": "X", "D": "X"}.get(name[0], "Y"), name[1])
        return groups[key]

    def target(name, at):
        kind = name[0]
        if kind == "D":
            return moved(at, "k", 1)
        axis = {"Z": "z", "X": "x", "B": "z"}.get(kind, "y")
        return moved(at, axis, SIGN[name[1] if kind[0] in "WB" else name[3]])

    def source(name, at):
        kind = name[0]
        if kind == "D":
            return moved(at, "k", 1)
        axis = {"Z": "z", "X": "x", "B": "z"}.get(kind, "y")
        return moved(at, axis, -SIGN[name[1] if kind[0] in "WB" else name[3]])

    def span(first, half):
        if half is None:
            return rows(first, 2 * TILE)
        return rows(first + half * TILE, TILE)

    def ends(name, at):
        kind = name[0]
        if kind == "B":
            ref = bits.at[moved(at, "z", -SIGN[name[1]] * (name[2] - 1))[1]]
            return ref, ref
        if kind == "W1":
            d = name[1]
            return far_ref.at[moved(at, "y", SIGN[d])[0]], wr.at[0 if d == "-" else 1]
        if kind == "W2a":
            h = 0 if name[1] == "+" else 1
            return far_ref.at[moved(at, "y", 2)[0], pl.ds(h * TILE, TILE)], stage.at[h]
        if kind == "W2b":
            h = 0 if name[1] == "+" else 1
            return stage.at[h], wr.at[2, pl.ds(h * TILE, TILE)]
        p, c, d = name[1:4]
        if kind == "Z":
            s = name[4]
            first = moved(at, "z", -SIGN[d] * (s - 1))[1] * (2 * TILE)
            half = None if s < NZ // 2 else (0 if d == "+" else 1)
            ref = xz[p][c].at[span(first, half)]
            return ref, ref
        if kind in "XD":
            whole = xr[p][c] if p < 2 else lg[0][c]
            if kind == "X":
                s = name[4]
                from_x = moved(at, "x", -SIGN[d] * (s - 1))[2]
                half = None if s < NX // 2 else (0 if d == "+" else 1)
            else:
                by, half = {"0": 0, "+": -1, "-": 1, "f": 2}[d], None
                from_x = moved(at, "x", by)[2]
            ref = whole.at[span((from_x * 2 + at[3]) * (2 * TILE), half)]
            return ref, ref
        i = 0 if d == "+" else 1
        top, low = pl.ds(i * TILE, TILE), pl.ds((1 - i) * TILE, TILE)
        if kind == "Y1":
            return p2[p][c].at[top], y1[p][c].at[i]
        if kind == "YA":
            return ps[p][c].at[i, top], yr[p][c].at[i, top]
        return ps[p][c].at[i, low], yr[p][c].at[i, low]

    def descriptor(name, at, to):
        src, dst = ends(name, at)
        return pltpu.make_async_remote_copy(
            src_ref=src, dst_ref=dst, send_sem=send_sem.at[group_of(name)], recv_sem=recv_sem.at[slot[arrives_with(name)]],
            device_id=device(to), device_id_type=MESH)

    def arrival(name):
        key = arrives_with(name)
        if len(together[key]) == 1:
            dst = ends(name, source(name, me))[1]
        else:
            kind, p, c = key
            dst = xr[0][c].at[pl.ds(0, {"D": 8, "Y": 4, "Y1": 2, "Z": 2, "X": 2}[kind] * TILE)]
        return pltpu.make_async_remote_copy(
            src_ref=dst, dst_ref=dst, send_sem=send_sem.at[0], recv_sem=recv_sem.at[slot[key]],
            device_id=device(source(name, me)), device_id_type=MESH)

    own_z = rows(me[1] * (2 * TILE), 2 * TILE)
    own_r = rows(r * (2 * TILE), 2 * TILE)

    def loads(c):
        piece = block_hbm.at[:, pl.ds(offsets[c], widths[c])]
        return (pltpu.make_async_copy(piece, xz[0][c].at[own_z], load_sem.at[c, 0]),
                pltpu.make_async_copy(piece, xr[0][c].at[own_r], load_sem.at[c, 1]))

    for c in range(chunks):
        for copy in loads(c):
            copy.start()
    send_copy = pltpu.make_async_copy(send_hbm, send_ref, misc_sem.at[0])
    degree_copy = pltpu.make_async_copy(degree_hbm, degree_ref, misc_sem.at[1])
    for copy in (send_copy, degree_copy):
        copy.start()
    peers = [moved(me, axis, by) for axis in "zyx" for by in (1, -1)] + [moved(me, "k", 1)]
    barrier = pltpu.get_barrier_semaphore()
    for peer in peers:
        pl.semaphore_signal(barrier, inc=1, device_id=device(peer), device_id_type=MESH)
    send_copy.wait()
    bits[me[1]] = jnp.zeros(bits.shape[1:], bits.dtype)
    bits[me[1], pl.ds(0, 1), pl.ds(0, NY * NZ)] = send_ref[...]
    pl.semaphore_wait(barrier, len(peers))

    def dot(a, b):
        return jnp.dot(a, b, preferred_element_type=jnp.float32)

    def widen(j):
        slot = "0+-2".index(j)
        out = pl.ds("2+-0".index(j) * 2 * TILE, 2 * TILE)
        y = moved(me, "y", {"0": 0, "+": 1, "-": -1, "2": 2}[j])[0]
        for z in range(NZ):
            told = bits[z, pl.ds(0, 1), :].astype(jnp.float32)
            lane = lax.broadcasted_iota(jnp.int32, told.shape, 1)
            bit = jnp.sum(jnp.where(lane == y * NZ + me[1], told, 0.0), axis=1, keepdims=True)
            if j == "0":
                piece = far_ref[me[0], :, pl.ds(z * TILE, TILE)]
            else:
                piece = wr[slot - 1, :, pl.ds(z * TILE, TILE)]
            piece = piece.astype(jnp.float32)
            wide[out, pl.ds(z * 2 * TILE, TILE)] = (piece * (1.0 - bit)).astype(jnp.bfloat16)
            wide[out, pl.ds(z * 2 * TILE + TILE, TILE)] = (piece * bit).astype(jnp.bfloat16)

    def run(name):
        kind = name[0]
        if kind == "L":
            for copy in loads(name[1]):
                copy.wait()
        elif kind == "E":
            widen(name[1])
        elif kind == "H":
            degree_copy.wait()
            for h in range(2):
                degrees = degree_ref[pl.ds(h, 1), :].astype(jnp.float32)
                div_ref[pl.ds(h * TILE, TILE), :] = jnp.broadcast_to(degrees, (TILE, TILE)).T
        elif kind == "C":
            p, c, j = name[1:]
            if j == "0":
                acc[p][c][...] = dot(wide[pl.ds(6 * TILE, 2 * TILE), :], xz[p][c][...])
            elif j == "2":
                p2[p][c][...] = dot(wide[pl.ds(0, 2 * TILE), :], xz[p][c][...]).astype(jnp.bfloat16)
            else:
                made = dot(wide[pl.ds(2 * TILE, 4 * TILE), :], xz[p][c][...])
                for i in range(2):
                    part = made[2 * i * TILE:(2 + 2 * i) * TILE]
                    pf[p][c][i] = part[i * TILE:(i + 1) * TILE]
                    ps[p][c][i, pl.ds((1 - i) * TILE, TILE)] = part[(1 - i) * TILE:(2 - i) * TILE].astype(jnp.bfloat16)
        elif kind == "R":
            p, c = name[1:]
            acc[p][c][...] += dot(row_ref[...], xr[p][c][...])
        elif kind == "A":
            p, c = name[1:]
            for i in range(2):
                ps[p][c][i, pl.ds(i * TILE, TILE)] = (pf[p][c][i] + y1[p][c][i].astype(jnp.float32)).astype(jnp.bfloat16)
        elif kind == "F":
            p, c = name[1:]
            summed = acc[p][c][...] + yr[p][c][0].astype(jnp.float32) + yr[p][c][1].astype(jnp.float32)
            divisor = jnp.concatenate([div_ref[...]] * (widths[c] // TILE), axis=1)
            power = (summed / divisor).astype(jnp.bfloat16)
            if p == 0:
                xz[1][c][own_z] = power
                xr[1][c][own_r] = power
            else:
                total = xr[1][c][own_r].astype(jnp.float32) + power.astype(jnp.float32)
                logs = jnp.log(jnp.maximum(3.0 * total, 1.0)).astype(jnp.bfloat16)
                lg[0][c][own_r] = logs
                logs_ref[:, pl.ds(offsets[c], widths[c])] = logs
        else:
            for c in range(chunks):
                first, count = offsets[c] // TILE, widths[c] // TILE

                @pl.when((r >= first) & (r < first + count))
                def _():
                    mine = pl.ds(pl.multiple_of((r - first) * TILE, TILE), TILE)
                    flip[...] = lg[0][c][:, mine].T

            for c in range(chunks):
                made = dot(flip[...], lg[0][c][...])
                gram_ref[:, pl.ds(offsets[c], widths[c])] = made * (1.0 / flip.shape[1])

    waited = set()
    for name in order:
        for dep in tasks[name][0]:
            if dep[0] == "got" and dep[1] not in waited:
                waited.update(together[arrives_with(dep[1])])
                arrival(dep[1]).wait_recv()
        if name in number:
            descriptor(name, me, target(name, me)).start()
        else:
            run(name)
    for key, i in groups.items():
        if key[0] == "W":
            sent = far_ref
        elif key[0] == "B":
            sent = bits.at[pl.ds(0, NZ - 1)]
        else:
            sent = wide.at[pl.ds(0, (3 if key[0] == "Y" else 7) * TILE)]
        pltpu.make_async_remote_copy(
            src_ref=sent, dst_ref=sent, send_sem=send_sem.at[i], recv_sem=recv_sem.at[0],
            device_id=device(moved(me, "k", 1)), device_id_type=MESH).wait_send()


def body(block, degree, tile_values, tile_rows, tile_cols, tile_count, send_tiles):
    near, far = build_dense(tile_rows, tile_cols, tile_count, tile_values)
    rows_here, features = block.shape
    widths = WIDTHS
    tasks = task_list(widths)
    names = list(tasks)
    order = [names[i] for i in ORDER]
    hbm = pl.BlockSpec(memory_space=pl.ANY)
    vmem = pl.BlockSpec(memory_space=pltpu.VMEM)
    column, ranks = NZ * 2 * TILE, 2 * NX
    bf16, f32 = jnp.bfloat16, jnp.float32

    def kernel(*refs):
        step_kernel(tasks, order, widths, *refs)

    def each(lead, dtype):
        return [pltpu.VMEM((*lead, w), dtype) for w in widths]

    both = [
        each((column,), bf16), each((ranks * 2 * TILE,), bf16), each((2 * TILE,), bf16), each((2, 2 * TILE), bf16),
        each((2, TILE), f32), each((2, TILE), bf16), each((2, 2 * TILE), bf16), each((2 * TILE,), f32),
    ]
    return pl.pallas_call(
        kernel,
        out_shape=(
            jax.ShapeDtypeStruct((rows_here, features), bf16),
            jax.ShapeDtypeStruct((features // ranks, features), f32),
        ),
        in_specs=[hbm, vmem, vmem, hbm, hbm],
        out_specs=(vmem, vmem),
        scratch_shapes=[
            [[b, b] for b in both] + [[each((ranks * 2 * TILE,), bf16)]],
            pltpu.VMEM((4 * 2 * TILE, column), bf16),
            pltpu.VMEM((3, 2 * TILE, NZ * TILE), bf16),
            pltpu.VMEM((2, TILE, NZ * TILE), bf16),
            pltpu.VMEM((NZ, 8, TILE), jnp.int32),
            pltpu.VMEM((TILE, ranks * 2 * TILE), bf16),
            pltpu.VMEM((1, NY * NZ), jnp.int32),
            pltpu.VMEM((2, TILE), jnp.int32),
            pltpu.VMEM((2 * TILE, TILE), f32),
            pltpu.SemaphoreType.DMA((len(widths), 2)),
            pltpu.SemaphoreType.DMA((2,)),
            pltpu.SemaphoreType.DMA((9,)),
            pltpu.SemaphoreType.DMA((13 * 2 * len(widths) + 4 * len(widths) + 13,)),
        ],
        compiler_params=pltpu.CompilerParams(
            collective_id=0, has_side_effects=True, vmem_limit_bytes=LIMIT),
    )(block, near, far, send_tiles, degree.reshape(2, TILE))


def solution(mesh):
    placed = (
        P(("grp", "row"), None),
        P(("grp", "row")),
        P(("grp", "row"), None, None),
        P(("grp", "row")),
        P(("grp", "row")),
        P(("grp", "row")),
        P(("grp", "row"), None),
    )
    return jax.shard_map(
        body,
        mesh=mesh,
        in_specs=placed,
        out_specs=(P(("grp", "row"), None), P(("grp", "row"), None)),
        check_vma=False,
    )
```

```python
import jax
import jax.numpy as jnp
from jax import lax
from jax.experimental import pallas as pl
from jax.experimental.pallas import tpu as pltpu
from jax.sharding import PartitionSpec as P

NX, NY, NZ = 4, 4, 8
TILE = 128
WIDTHS = (256, 256, 256, 128, 128)
BACKLOG = 0.5
RATE = 460e6
LIMIT = 46 * 1024 * 1024
BUILD_LIMIT = 20 * 1024 * 1024
BITS_LATE = 4.0
LATE = {"z": 2.3, "y": 2.8, "x": 5.0, "d": 4.0, "X": 2.5, "D": 1.5}
MESH = pl.DeviceIdType.MESH
ORDER = (
    18, 19, 23, 11, 27, 134, 4, 105, 0, 47, 52, 8, 60, 114, 48, 135, 1, 12, 110, 76, 20, 24, 5, 7, 58, 9, 31, 53,
    143, 87, 147, 2, 29, 10, 49, 81, 106, 145, 85, 115, 56, 21, 6, 13, 25, 119, 86, 50, 116, 54, 30, 3, 77, 89, 118, 90,
    57, 22, 26, 59, 14, 82, 146, 107, 51, 33, 28, 120, 15, 55, 144, 111, 16, 32, 88, 78, 117, 17, 35, 139, 43, 37, 36, 40,
    83, 108, 64, 69, 136, 41, 72, 34, 112, 63, 79, 44, 65, 39, 140, 42, 45, 73, 38, 109, 92, 70, 62, 148, 84, 68, 71, 137,
    74, 113, 141, 80, 66, 61, 46, 173, 167, 163, 67, 75, 191, 122, 195, 91, 93, 199, 101, 138, 201, 98, 127, 142, 94, 168, 124, 164,
    99, 102, 123, 121, 196, 97, 100, 103, 192, 130, 175, 151, 171, 152, 156, 200, 131, 153, 165, 169, 204, 203, 95, 96, 104, 223, 150, 159,
    149, 126, 174, 219, 197, 193, 172, 129, 154, 177, 166, 125, 229, 128, 227, 132, 155, 170, 158, 161, 202, 224, 157, 160, 220, 198, 133, 251,
    194, 255, 247, 228, 162, 230, 180, 275, 205, 179, 279, 283, 285, 187, 184, 257, 206, 232, 221, 225, 188, 185, 207, 212, 215, 208, 248, 252,
    233, 178, 234, 181, 176, 183, 186, 261, 260, 284, 189, 258, 213, 276, 216, 280, 209, 222, 226, 211, 286, 214, 217, 210, 249, 253, 256, 182,
    190, 281, 287, 303, 277, 305, 235, 240, 243, 250, 254, 218, 313, 311, 236, 244, 241, 278, 282, 237, 262, 288, 263, 268, 271, 306, 304, 239,
    242, 245, 264, 291, 299, 259, 296, 272, 231, 269, 314, 312, 292, 289, 297, 267, 270, 273, 300, 238, 246, 319, 321, 295, 301, 298, 265, 290,
    266, 318, 309, 316, 310, 274, 327, 329, 293, 294, 302, 337, 335, 322, 325, 308, 307, 320, 330, 328, 336, 338, 340, 323, 339, 315, 317, 341,
    332, 326, 333, 324, 331, 334, 342, 343,
)
SIGN = {"+": 1, "-": -1}


def build_kernel(cell_s, count_s, values, row_ref, far_ref, cells):
    codes = cells.shape[0] // 2

    def clear(c, carry):
        for r in range(2):
            cells[r * codes + c] = jnp.zeros((TILE, TILE), jnp.float32)
        return carry

    lax.fori_loop(0, codes, clear, 0)

    def add(s, carry):
        cell = cell_s[s]
        cells[cell] = cells[cell] + values[s].astype(jnp.float32)
        return carry

    lax.fori_loop(0, count_s[0], add, 0)
    local = codes - NY * NZ
    for r in range(2):
        rows = pl.ds(r * TILE, TILE)
        for c in range(local):
            row_ref[rows, pl.ds(c * TILE, TILE)] = cells[r * codes + c].astype(jnp.bfloat16)
        for y in range(NY):
            for z in range(NZ):
                far_ref[y, rows, pl.ds(z * TILE, TILE)] = cells[r * codes + local + y * NZ + z].astype(jnp.bfloat16)


def build_dense(tile_rows, tile_cols, tile_count, tile_values):
    codes = 2 * 2 * NX + NY * NZ
    smem = pl.BlockSpec(memory_space=pltpu.SMEM)
    vmem = pl.BlockSpec(memory_space=pltpu.VMEM)
    return pl.pallas_call(
        build_kernel,
        out_shape=(
            jax.ShapeDtypeStruct((2 * TILE, 4 * NX * TILE), jnp.bfloat16),
            jax.ShapeDtypeStruct((NY, 2 * TILE, NZ * TILE), jnp.bfloat16),
        ),
        in_specs=[smem, smem, vmem],
        out_specs=(vmem, vmem),
        scratch_shapes=[pltpu.VMEM((2 * codes, TILE, TILE), jnp.float32)],
        compiler_params=pltpu.CompilerParams(vmem_limit_bytes=BUILD_LIMIT),
    )(tile_rows * codes + tile_cols, tile_count, tile_values)


def task_list(widths):
    tasks = {}
    chunks = len(widths)

    def task(name, deps, link=None, units=0.0, cost=0.05, rank=0):
        late = LATE.get("X" if name[0] == "X" and name[1] == 2 else "D" if name[0] == "D" and name[1] == 2 else (link or "z")[0])
        late = BITS_LATE if name[0] == "B" else late
        tasks[name] = (deps, link, units, cost, rank, late)

    def got(name):
        return ("got", name)

    hops = [("B", d, s) for d in "+-" for s in range(1, NZ // 2 + (d == "+"))]
    for _, d, s in hops:
        task(("B", d, s), [] if s == 1 else [got(("B", d, s - 1))], "z" + d, 0.01, 0.05, -20)
    task(("H",), [], None, 0, 0.3, 50)
    for d in "+-":
        task(("W2a", d), [], "y" + d, 1, 0.05, -11)
        task(("W1", d), [], "y" + d, 2, 0.05, -10)
        task(("W2b", d), [got(("W2a", d))], "y" + d, 1, 0.05, -10)
    bits = [got(hop) for hop in hops] + [("H",)]
    task(("E", "0"), bits, None, 0, 0.4, -5)
    task(("E", "+"), bits + [got(("W1", "-"))], None, 0, 0.4, -5)
    task(("E", "-"), bits + [got(("W1", "+"))], None, 0, 0.4, -5)
    task(("E", "2"), bits + [got(("W2b", "+")), got(("W2b", "-"))], None, 0, 0.4, -5)
    gram_deps = []
    for p in range(3):
        for c in range(chunks):
            rank = p * chunks + c
            part = widths[c] / sum(widths)
            product = 2 * (2 * TILE) * (NZ * 2 * TILE) * max(widths[c], 190) / RATE
            own = [("L", c)] if p == 0 else [("F", p - 1, c)]
            if p == 0:
                task(("L", c), [], None, 0, 0.05, rank)

            def ring(kind, axis, size):
                half = size // 2
                for d in "+-":
                    for s in range(1, half + 1):
                        deps = own if s == 1 else [got((kind, p, c, d, s - 1))]
                        task((kind, p, c, d, s), deps, axis + d, (2 if s < half else 1) * part, 0.05, rank)
                return [got((kind, p, c, d, s)) for d in "+-" for s in range(1, half + 1)]

            column = ring("Z", "z", NZ) + own if p < 2 else []
            row = ring("X", "x", NX) + own
            for q, deps, units in (
                ("0", own, 2),
                ("+", [got(("X", p, c, "+", 1))], 2),
                ("-", [got(("X", p, c, "-", 1))], 2),
                ("f", [got(("X", p, c, "+", 2)), got(("X", p, c, "-", 2))], 2),
            ):
                task(("D", p, c, q), deps, "d", units * part, 0.05, rank)
                row.append(got(("D", p, c, q)))
            if p == 2:
                gram_deps += row
                continue
            task(("C", p, c, "2"), column + [("E", "2")], None, 0, product, rank)
            task(("C", p, c, "s"), column + [("E", j) for j in "+-"], None, 0, 2.1 * product, rank)
            task(("C", p, c, "0"), column + [("E", "0")], None, 0, product * 0.95, rank)
            task(("R", p, c), row + [("C", p, c, "0"), ("H",)], None, 0, product * 1.2, rank)
            arrived = []
            crossed = [got(("Y1", p, c, d)) for d in "+-"]
            task(("A", p, c), crossed + [("C", p, c, "s")], None, 0, 0.1, rank)
            for d in "+-":
                task(("Y1", p, c, d), [("C", p, c, "2")], "y" + d, part, 0.05, rank)
                task(("YB", p, c, d), [("C", p, c, "s")], "y" + d, part, 0.05, rank)
                task(("YA", p, c, d), [("A", p, c)], "y" + d, part, 0.05, rank)
                arrived += [got(("YB", p, c, d)), got(("YA", p, c, d))]
            task(("F", p, c), arrived + [("R", p, c), ("H",)] + own, None, 0, 0.15, rank)
    task(("G",), gram_deps, None, 0, 0.95, 99)
    return tasks


def task_order(tasks, backlog):
    unit = 5.62
    now, free, ended, landed, order = 3.0, {}, {}, {}, []
    left = dict(tasks)
    while left:
        best, best_key, soonest = None, None, 1e9
        for name, (deps, link, units, cost, rank, late) in left.items():
            ready = 0.0
            for dep in deps:
                at = landed.get(dep[1]) if dep[0] == "got" else ended.get(dep)
                if at is None:
                    ready = None
                    break
                ready = max(ready, at)
            if ready is None:
                continue
            if link is not None:
                ready = max(ready, free.get(link, 0.0) - backlog)
            if ready <= now + 1e-9:
                key = (link is None, rank, ready)
                if best is None or key < best_key:
                    best, best_key = name, key
            else:
                soonest = min(soonest, ready)
        if best is None:
            now = soonest
            continue
        deps, link, units, cost, rank, late = left.pop(best)
        now += cost
        ended[best] = now
        if link is not None:
            took = units * unit * (0.07 if link == "d" else 1.0)
            free[link] = max(now, free.get(link, 0.0)) + took
            landed[best] = free[link] + late
        order.append(best)
    return order, now


def step_kernel(tasks, order, widths, block_hbm, row_ref, far_ref, send_hbm, degree_hbm, logs_ref, gram_ref,
                per_chunk, wide, wr, stage, bits, flip, send_ref, degree_ref, div_ref,
                load_sem, misc_sem, send_sem, recv_sem):
    chunks = len(widths)
    offsets = [sum(widths[:c]) for c in range(chunks)]
    xz, xr, p2, ps, pf, y1, yr, acc, lg = per_chunk
    g, r = lax.axis_index("grp"), lax.axis_index("row")
    me = (lax.div(g, NZ), lax.rem(g, NZ), lax.div(r, 2), lax.rem(r, 2))

    def moved(at, axis, by):
        y, z, x, k = at
        if axis == "y":
            return (lax.rem(y + by + NY, NY), z, x, k)
        if axis == "z":
            return (y, lax.rem(z + by + NZ, NZ), x, k)
        if axis == "x":
            return (y, z, lax.rem(x + by + NX, NX), k)
        return (y, z, x, 1 - k)

    def device(at):
        return (at[0] * NZ + at[1], at[2] * 2 + at[3])

    def rows(first, size):
        return pl.ds(pl.multiple_of(first, TILE), size)

    number = {}
    for name in tasks:
        if tasks[name][1] is not None:
            number[name] = len(number)

    def arrives_with(name):
        if name[0] == "D":
            return ("D", name[1], name[2])
        if name[0] == "Y1":
            return ("Y1", name[1], name[2])
        if name[0] in ("YA", "YB"):
            return ("Y", name[1], name[2])
        if (name[0], name[-1]) in (("Z", NZ // 2), ("X", NX // 2)):
            return (name[0], name[1], name[2])
        return name

    together = {}
    for name in number:
        together.setdefault(arrives_with(name), []).append(name)
    slot = {key: i for i, key in enumerate(together)}
    groups = {}
    for name in number:
        key = (name[0][0],) if name[0][0] in "WB" else ({"Z": "Z", "X": "X", "D": "X"}.get(name[0], "Y"), name[1])
        groups.setdefault(key, len(groups))

    def group_of(name):
        key = (name[0][0],) if name[0][0] in "WB" else ({"Z": "Z", "X": "X", "D": "X"}.get(name[0], "Y"), name[1])
        return groups[key]

    def target(name, at):
        kind = name[0]
        if kind == "D":
            return moved(at, "k", 1)
        axis = {"Z": "z", "X": "x", "B": "z"}.get(kind, "y")
        return moved(at, axis, SIGN[name[1] if kind[0] in "WB" else name[3]])

    def source(name, at):
        kind = name[0]
        if kind == "D":
            return moved(at, "k", 1)
        axis = {"Z": "z", "X": "x", "B": "z"}.get(kind, "y")
        return moved(at, axis, -SIGN[name[1] if kind[0] in "WB" else name[3]])

    def span(first, half):
        if half is None:
            return rows(first, 2 * TILE)
        return rows(first + half * TILE, TILE)

    def ends(name, at):
        kind = name[0]
        if kind == "B":
            ref = bits.at[moved(at, "z", -SIGN[name[1]] * (name[2] - 1))[1]]
            return ref, ref
        if kind == "W1":
            d = name[1]
            return far_ref.at[moved(at, "y", SIGN[d])[0]], wr.at[0 if d == "-" else 1]
        if kind == "W2a":
            h = 0 if name[1] == "+" else 1
            return far_ref.at[moved(at, "y", 2)[0], pl.ds(h * TILE, TILE)], stage.at[h]
        if kind == "W2b":
            h = 0 if name[1] == "+" else 1
            return stage.at[h], wr.at[2, pl.ds(h * TILE, TILE)]
        p, c, d = name[1:4]
        if kind == "Z":
            s = name[4]
            first = moved(at, "z", -SIGN[d] * (s - 1))[1] * (2 * TILE)
            half = None if s < NZ // 2 else (0 if d == "+" else 1)
            ref = xz[p][c].at[span(first, half)]
            return ref, ref
        if kind in "XD":
            whole = xr[p][c] if p < 2 else lg[0][c]
            if kind == "X":
                s = name[4]
                from_x = moved(at, "x", -SIGN[d] * (s - 1))[2]
                half = None if s < NX // 2 else (0 if d == "+" else 1)
            else:
                by, half = {"0": 0, "+": -1, "-": 1, "f": 2}[d], None
                from_x = moved(at, "x", by)[2]
            ref = whole.at[span((from_x * 2 + at[3]) * (2 * TILE), half)]
            return ref, ref
        i = 0 if d == "+" else 1
        top, low = pl.ds(i * TILE, TILE), pl.ds((1 - i) * TILE, TILE)
        if kind == "Y1":
            return p2[p][c].at[top], y1[p][c].at[i]
        if kind == "YA":
            return ps[p][c].at[i, top], yr[p][c].at[i, top]
        return ps[p][c].at[i, low], yr[p][c].at[i, low]

    def descriptor(name, at, to):
        src, dst = ends(name, at)
        return pltpu.make_async_remote_copy(
            src_ref=src, dst_ref=dst, send_sem=send_sem.at[group_of(name)], recv_sem=recv_sem.at[slot[arrives_with(name)]],
            device_id=device(to), device_id_type=MESH)

    def arrival(name):
        key = arrives_with(name)
        if len(together[key]) == 1:
            dst = ends(name, source(name, me))[1]
        else:
            kind, p, c = key
            dst = xr[0][c].at[pl.ds(0, {"D": 8, "Y": 4, "Y1": 2, "Z": 2, "X": 2}[kind] * TILE)]
        return pltpu.make_async_remote_copy(
            src_ref=dst, dst_ref=dst, send_sem=send_sem.at[0], recv_sem=recv_sem.at[slot[key]],
            device_id=device(source(name, me)), device_id_type=MESH)

    own_z = rows(me[1] * (2 * TILE), 2 * TILE)
    own_r = rows(r * (2 * TILE), 2 * TILE)

    def loads(c):
        piece = block_hbm.at[:, pl.ds(offsets[c], widths[c])]
        return (pltpu.make_async_copy(piece, xz[0][c].at[own_z], load_sem.at[c, 0]),
                pltpu.make_async_copy(piece, xr[0][c].at[own_r], load_sem.at[c, 1]))

    for c in range(chunks):
        for copy in loads(c):
            copy.start()
    send_copy = pltpu.make_async_copy(send_hbm, send_ref, misc_sem.at[0])
    degree_copy = pltpu.make_async_copy(degree_hbm, degree_ref, misc_sem.at[1])
    for copy in (send_copy, degree_copy):
        copy.start()
    peers = [moved(me, axis, by) for axis in "zyx" for by in (1, -1)] + [moved(me, "k", 1)]
    barrier = pltpu.get_barrier_semaphore()
    for peer in peers:
        pl.semaphore_signal(barrier, inc=1, device_id=device(peer), device_id_type=MESH)
    send_copy.wait()
    bits[me[1]] = jnp.zeros(bits.shape[1:], bits.dtype)
    bits[me[1], pl.ds(0, 1), pl.ds(0, NY * NZ)] = send_ref[...]
    pl.semaphore_wait(barrier, len(peers))

    def dot(a, b):
        return jnp.dot(a, b, preferred_element_type=jnp.float32)

    def widen(j):
        slot = "0+-2".index(j)
        out = pl.ds("2+-0".index(j) * 2 * TILE, 2 * TILE)
        y = moved(me, "y", {"0": 0, "+": 1, "-": -1, "2": 2}[j])[0]
        for z in range(NZ):
            told = bits[z, pl.ds(0, 1), :].astype(jnp.float32)
            lane = lax.broadcasted_iota(jnp.int32, told.shape, 1)
            bit = jnp.sum(jnp.where(lane == y * NZ + me[1], told, 0.0), axis=1, keepdims=True)
            if j == "0":
                piece = far_ref[me[0], :, pl.ds(z * TILE, TILE)]
            else:
                piece = wr[slot - 1, :, pl.ds(z * TILE, TILE)]
            piece = piece.astype(jnp.float32)
            wide[out, pl.ds(z * 2 * TILE, TILE)] = (piece * (1.0 - bit)).astype(jnp.bfloat16)
            wide[out, pl.ds(z * 2 * TILE + TILE, TILE)] = (piece * bit).astype(jnp.bfloat16)

    def run(name):
        kind = name[0]
        if kind == "L":
            for copy in loads(name[1]):
                copy.wait()
        elif kind == "E":
            widen(name[1])
        elif kind == "H":
            degree_copy.wait()
            for h in range(2):
                degrees = degree_ref[pl.ds(h, 1), :].astype(jnp.float32)
                div_ref[pl.ds(h * TILE, TILE), :] = jnp.broadcast_to(degrees, (TILE, TILE)).T
        elif kind == "C":
            p, c, j = name[1:]
            if j == "0":
                acc[p][c][...] = dot(wide[pl.ds(6 * TILE, 2 * TILE), :], xz[p][c][...])
            elif j == "2":
                p2[p][c][...] = dot(wide[pl.ds(0, 2 * TILE), :], xz[p][c][...]).astype(jnp.bfloat16)
            else:
                made = dot(wide[pl.ds(2 * TILE, 4 * TILE), :], xz[p][c][...])
                for i in range(2):
                    part = made[2 * i * TILE:(2 + 2 * i) * TILE]
                    pf[p][c][i] = part[i * TILE:(i + 1) * TILE]
                    ps[p][c][i, pl.ds((1 - i) * TILE, TILE)] = part[(1 - i) * TILE:(2 - i) * TILE].astype(jnp.bfloat16)
        elif kind == "R":
            p, c = name[1:]
            acc[p][c][...] += dot(row_ref[...], xr[p][c][...])
        elif kind == "A":
            p, c = name[1:]
            for i in range(2):
                ps[p][c][i, pl.ds(i * TILE, TILE)] = (pf[p][c][i] + y1[p][c][i].astype(jnp.float32)).astype(jnp.bfloat16)
        elif kind == "F":
            p, c = name[1:]
            summed = acc[p][c][...] + yr[p][c][0].astype(jnp.float32) + yr[p][c][1].astype(jnp.float32)
            divisor = jnp.concatenate([div_ref[...]] * (widths[c] // TILE), axis=1)
            power = (summed / divisor).astype(jnp.bfloat16)
            if p == 0:
                xz[1][c][own_z] = power
                xr[1][c][own_r] = power
            else:
                total = xr[1][c][own_r].astype(jnp.float32) + power.astype(jnp.float32)
                logs = jnp.log(jnp.maximum(3.0 * total, 1.0)).astype(jnp.bfloat16)
                lg[0][c][own_r] = logs
                logs_ref[:, pl.ds(offsets[c], widths[c])] = logs
        else:
            for c in range(chunks):
                first, count = offsets[c] // TILE, widths[c] // TILE

                @pl.when((r >= first) & (r < first + count))
                def _():
                    mine = pl.ds(pl.multiple_of((r - first) * TILE, TILE), TILE)
                    flip[...] = lg[0][c][:, mine].T

            for c in range(chunks):
                made = dot(flip[...], lg[0][c][...])
                gram_ref[:, pl.ds(offsets[c], widths[c])] = made * (1.0 / flip.shape[1])

    waited = set()
    for name in order:
        for dep in tasks[name][0]:
            if dep[0] == "got" and dep[1] not in waited:
                waited.update(together[arrives_with(dep[1])])
                arrival(dep[1]).wait_recv()
        if name in number:
            descriptor(name, me, target(name, me)).start()
        else:
            run(name)
    for key, i in groups.items():
        if key[0] == "W":
            sent = far_ref
        elif key[0] == "B":
            sent = bits.at[pl.ds(0, NZ - 1)]
        else:
            sent = wide.at[pl.ds(0, (3 if key[0] == "Y" else 7) * TILE)]
        pltpu.make_async_remote_copy(
            src_ref=sent, dst_ref=sent, send_sem=send_sem.at[i], recv_sem=recv_sem.at[0],
            device_id=device(moved(me, "k", 1)), device_id_type=MESH).wait_send()


def body(block, degree, tile_values, tile_rows, tile_cols, tile_count, send_tiles):
    near, far = build_dense(tile_rows, tile_cols, tile_count, tile_values)
    rows_here, features = block.shape
    widths = WIDTHS
    tasks = task_list(widths)
    names = list(tasks)
    order = [names[i] for i in ORDER]
    hbm = pl.BlockSpec(memory_space=pl.ANY)
    vmem = pl.BlockSpec(memory_space=pltpu.VMEM)
    column, ranks = NZ * 2 * TILE, 2 * NX
    bf16, f32 = jnp.bfloat16, jnp.float32

    def kernel(*refs):
        step_kernel(tasks, order, widths, *refs)

    def each(lead, dtype):
        return [pltpu.VMEM((*lead, w), dtype) for w in widths]

    both = [
        each((column,), bf16), each((ranks * 2 * TILE,), bf16), each((2 * TILE,), bf16), each((2, 2 * TILE), bf16),
        each((2, TILE), f32), each((2, TILE), bf16), each((2, 2 * TILE), bf16), each((2 * TILE,), f32),
    ]
    return pl.pallas_call(
        kernel,
        out_shape=(
            jax.ShapeDtypeStruct((rows_here, features), bf16),
            jax.ShapeDtypeStruct((features // ranks, features), f32),
        ),
        in_specs=[hbm, vmem, vmem, hbm, hbm],
        out_specs=(vmem, vmem),
        scratch_shapes=[
            [[b, b] for b in both] + [[each((ranks * 2 * TILE,), bf16)]],
            pltpu.VMEM((4 * 2 * TILE, column), bf16),
            pltpu.VMEM((3, 2 * TILE, NZ * TILE), bf16),
            pltpu.VMEM((2, TILE, NZ * TILE), bf16),
            pltpu.VMEM((NZ, 8, TILE), jnp.int32),
            pltpu.VMEM((TILE, ranks * 2 * TILE), bf16),
            pltpu.VMEM((1, NY * NZ), jnp.int32),
            pltpu.VMEM((2, TILE), jnp.int32),
            pltpu.VMEM((2 * TILE, TILE), f32),
            pltpu.SemaphoreType.DMA((len(widths), 2)),
            pltpu.SemaphoreType.DMA((2,)),
            pltpu.SemaphoreType.DMA((9,)),
            pltpu.SemaphoreType.DMA((13 * 2 * len(widths) + 4 * len(widths) + 13,)),
        ],
        compiler_params=pltpu.CompilerParams(
            collective_id=0, has_side_effects=True, vmem_limit_bytes=LIMIT),
    )(block, near, far, send_tiles, degree.reshape(2, TILE))


def solution(mesh):
    placed = (
        P(("grp", "row"), None),
        P(("grp", "row")),
        P(("grp", "row"), None, None),
        P(("grp", "row")),
        P(("grp", "row")),
        P(("grp", "row")),
        P(("grp", "row"), None),
    )
    return jax.shard_map(
        body,
        mesh=mesh,
        in_specs=placed,
        out_specs=(P(("grp", "row"), None), P(("grp", "row"), None)),
        check_vma=False,
    )
```
